128 devices in a mesh: grp: 8 (over z, y_hi), tm: 16 (over x, y_lo, core).
Axes of the slice: x: 4, y: 4 (y_hi: 2, y_lo: 2; y = y_hi * 2 + y_lo), z: 4, core: 2. Of those that a mesh axis runs over, the one named last changes fastest.
Arguments:
- initial: float32 [16, 16384], P('grp'), parts along dimension 0, may hold values from -1 to 1
- forcing: float32 [16, 64, 16384], P('grp', 'tm'), parts along dimension 0, may hold values from -1.8 to 1.8
- fine_blocks: float32 [16, 3, 128, 128], replicated, may hold values from -0.2 to 0.9, as said below
- coarse_blocks: float32 [16, 3, 128, 128], replicated, may hold values from -0.2 to 0.9, as said below
Outputs:
- solution: float32 [16, 64, 16384], P('grp', 'tm'), parts along dimension 0
The draws below stay inside these ranges and needn't reach their ends.
There are 8 independent parts, one for each index of `grp`. The reference program is written for one: setup_inputs(seed, part) draws one part's arguments, and reference() takes and returns one part's arrays. A program takes and returns all parts, laid end to end along the dimension named above; an argument that names none is the same for every part. Nothing has to cross between parts.
Inputs may be any that keep to these rules, and one draw needn't show every extreme that they name: `fine_blocks`: 16 x 3 blocks of 128 x 128. `coarse_blocks`: 16 x 3 blocks of 128 x 128.
All inputs are finite; a program needn't handle non-finite values.
Results may differ from the reference program's by a relative error of at most 0.00013.
Values sent between devices are 32-bit elements; how exact they have to be, the bound alone decides.
No kernel may reach another device: no remote copies, remote signals or barrier semaphores. Data moves between devices by JAX's collectives and lax.ppermute only.
A program may use at most 64 MiB of HBM per device.

```python
import math
import jax
import jax.numpy as jnp
from jax import lax

W = 16384
BLK = 128
ZONES = 16
INST = 2
M = 4
ITERS = 1
NT = 64


def make_blocks(key, centre):
    noise = jnp.clip(jax.random.normal(key, (ZONES, 3, BLK, BLK), jnp.float32), -4.0, 4.0)
    noise = noise / math.sqrt(BLK)
    weights = jnp.array([0.12, 0.25, 0.12], jnp.float32)[None, :, None, None]
    middle = jnp.array([0.0, 1.0, 0.0], jnp.float32)[None, :, None, None]
    return noise * weights + centre * middle * jnp.eye(BLK, dtype=jnp.float32)[None, None]


def draw_fine_blocks(key, part):
    return make_blocks(jax.random.fold_in(key, 11), 0.7)


def draw_coarse_blocks(key, part):
    return make_blocks(jax.random.fold_in(key, 23), 0.65)


def levels(stream_key, shape, split, low, top_value):
    gain = 1.0
    for position, parts in split:
        steps = jax.random.uniform(jax.random.fold_in(jax.random.fold_in(stream_key, 6), position), (parts,), jnp.float32, low / len(split), top_value / len(split))
        gain = gain * jnp.repeat(jnp.exp(steps), shape[position] // parts).reshape((-1,) + (1,) * (len(shape) - 1 - position))
    return gain


def normal_values(rng, extent, deviation, reach, pieces=(), kind=jnp.bfloat16):
    gain = levels(rng, extent, pieces, -0.22, 0.18) if pieces else 1.0
    values = jax.random.normal(rng, extent, jnp.float32) * deviation * gain
    return jnp.minimum(jnp.maximum(values, -reach), reach).astype(kind)


def setup_inputs(seed: int = 0, part: int = 0) -> dict:
    streams_of = jax.random.split(jax.random.key(seed), 5)
    own_keys = jax.random.split(jax.random.fold_in(streams_of[4], part), 5)
    initial = jnp.clip(jax.random.uniform(own_keys[0], (INST, W), jnp.float32, -1.0, 1.0), -1.0, 1.0)
    forcing = normal_values(own_keys[1], (INST, NT, W), 0.3, 1.8, ((1, 16),), jnp.float32)
    fine_blocks = draw_fine_blocks(jax.random.fold_in(streams_of[4], 71), part)
    coarse_blocks = draw_coarse_blocks(jax.random.fold_in(streams_of[4], 71), part)
    return {"initial": initial, "forcing": forcing, "fine_blocks": fine_blocks, "coarse_blocks": coarse_blocks}


DELTA = 0.05


def propagate(states, blocks, delta_t):
    layout = states.shape
    block_size = blocks.shape[-1]
    zone_count = blocks.shape[0]
    grouped = states.reshape(-1, layout[-1] // block_size, block_size)
    border = jnp.zeros_like(grouped[:, :1])
    left_side = jnp.concatenate([border, grouped[:, :-1]], axis=1)
    right_side = jnp.concatenate([grouped[:, 1:], border], axis=1)
    stacked = jnp.stack([left_side, grouped, right_side]).reshape(3, grouped.shape[0], -1, zone_count, block_size)
    mixing = jnp.einsum("kbrzn,zkmn->brzm", stacked, blocks, precision=lax.Precision.HIGHEST).reshape(layout)
    solved = mixing
    for _ in range(2):
        cubed_part = solved * solved * solved
        solved = solved - (solved - delta_t * (solved - cubed_part) - mixing) / (1.0 - delta_t + 3.0 * delta_t * solved * solved)
    return solved


def sweep(current, forcing_grid, carried, blocks, want_next):
    running = carried
    columns = []
    for slot in range(current.shape[2] - 1):
        running = propagate(running, blocks, DELTA) + forcing_grid[:, :, slot]
        columns.append(running)
    columns.append(current[:, :, -1])
    updated = jnp.stack(columns, axis=2)
    following = propagate(running, blocks, DELTA) + forcing_grid[:, :, -1] if want_next else None
    return updated, following


def coarse_chain(start, rhs_values, blocks, coarse_dt):
    def advance(carry_state, source):
        stepped = propagate(carry_state, blocks, coarse_dt) + source
        return stepped, stepped
    _, history = lax.scan(advance, start, jnp.moveaxis(rhs_values, 1, 0))
    return jnp.moveaxis(history, 0, 1)


def reference(initial, forcing, fine_blocks, coarse_blocks):
    members = forcing.shape[0]
    grid_cells = forcing.shape[2]
    forcing_grid = forcing.reshape(members, -1, M, grid_cells)
    current = jnp.zeros(forcing_grid.shape, jnp.float32)

    def carried_in(values):
        return jnp.concatenate([initial[:, None], values[:, :-1, -1]], axis=1)

    current, _ = sweep(current, forcing_grid, carried_in(current), fine_blocks, False)
    for _ in range(ITERS):
        corner = propagate(current[:, :, -2], fine_blocks, DELTA) + forcing_grid[:, :, -1]
        current = jnp.concatenate([current[:, :, :-1], corner[:, :, None]], axis=2)
        carried = carried_in(current)
        current, following = sweep(current, forcing_grid, carried, fine_blocks, True)
        coarse_rhs = following - propagate(carried, coarse_blocks, DELTA * M)
        coarse_vals = coarse_chain(initial, coarse_rhs, coarse_blocks, DELTA * M)
        current = jnp.concatenate([current[:, :, :-1], coarse_vals[:, :, None]], axis=2)
        current, _ = sweep(current, forcing_grid, carried_in(current), fine_blocks, False)
    return current.reshape(members, -1, grid_cells)
```

```python
import functools

import jax
import jax.numpy as jnp
from jax import lax
from jax.experimental import pallas as pl
from jax.experimental.pallas import tpu as pltpu
from jax.sharding import PartitionSpec as P

M = 4
DELTA = 0.05
BLK = 128
BF16 = jnp.bfloat16
F32 = jnp.float32


def split(value):
    high = value.astype(BF16)
    low = (value - high.astype(F32)).astype(BF16)
    return jnp.concatenate([high, low], axis=0)


def shifted(value, down):
    parts = []
    for part in jnp.split(value, value.shape[0] // 8, axis=0):
        rows = lax.broadcasted_iota(jnp.int32, part.shape, 0)
        moved = pltpu.roll(part, 1 if down else 7, axis=0)
        parts.append(jnp.where(rows == (0 if down else 7), 0.0, moved))
    return jnp.concatenate(parts, axis=0)


def put(state_ref, zone, value):
    zones = state_ref.shape[0] - 2
    state_ref[zone + 1] = split(value)
    if zone == zones - 1:
        state_ref[0] = split(shifted(value, True))
    if zone == 0:
        state_ref[zones + 1] = split(shifted(value, False))


def solve(mixing, step):
    solved = mixing
    for _ in range(2):
        squared = solved * solved
        solved = (mixing + (2.0 * step * solved) * squared) / ((1.0 - step) + (3.0 * step) * squared)
    return solved


def propagate_zone(state_ref, weights_ref, zone, step):
    rows = state_ref.shape[1] // 2
    lhs = jnp.concatenate([state_ref[zone], state_ref[zone + 1], state_ref[zone + 2]], axis=1)
    product = jnp.dot(lhs, weights_ref[zone], preferred_element_type=F32)
    low, high = product[rows:], product[:rows]
    mixing = high[:, :BLK] + (high[:, BLK:] + (low[:, :BLK] + low[:, BLK:]))
    return solve(mixing, step)


def zone_order(zones, start):
    return [(start + i) % zones for i in range(zones)]


def prepare_kernel(blocks_ref, out_ref):
    for k in range(3):
        turned = blocks_ref[0, k].T
        high = turned.astype(BF16)
        out_ref[0, k * BLK:(k + 1) * BLK, :BLK] = high
        out_ref[0, k * BLK:(k + 1) * BLK, BLK:] = (turned - high.astype(F32)).astype(BF16)


def prepare(blocks):
    zones = blocks.shape[0]
    return pl.pallas_call(
        prepare_kernel,
        grid=(zones,),
        in_specs=[pl.BlockSpec((1, 3, BLK, BLK), lambda z: (z, 0, 0, 0))],
        out_specs=pl.BlockSpec((1, 3 * BLK, 2 * BLK), lambda z: (z, 0, 0)),
        out_shape=jax.ShapeDtypeStruct((zones, 3 * BLK, 2 * BLK), BF16),
        name="prepare",
    )(blocks)


VMEM = pl.BlockSpec(memory_space=pltpu.VMEM)
SMEM = pl.BlockSpec(memory_space=pltpu.SMEM)


def force_rows(force_ref, zone, slot):
    per = force_ref.shape[0] // 2
    zones = per // (M * 8)
    return jnp.concatenate(
        [force_ref[pl.ds(i * per + zone * M + slot, 8, stride=zones * M), :] for i in range(2)], axis=0
    )


def first_rows(initial_ref, zone):
    zones = initial_ref.shape[0] // 16
    return jnp.concatenate([initial_ref[pl.ds(zone * 2 + i, 8, stride=zones * 2), :] for i in range(2)], axis=0)


def relax_kernel(place_ref, initial_ref, force_ref, weights_ref, out_ref, state_a, state_b):
    zones = weights_ref.shape[0]
    leading = place_ref[0] == 0
    for z in range(zones):
        put(state_a, z, force_rows(force_ref, z, 0))

    @pl.when(leading)
    def _():
        for z in range(zones):
            put(state_b, z, first_rows(initial_ref, z))
        for z in range(zones):
            put(state_a, z, propagate_zone(state_b, weights_ref, z, DELTA) + force_rows(force_ref, z, 0))

    source, target = state_a, state_b
    for slot in range(1, M):
        for z in zone_order(zones, slot - 1):
            value = propagate_zone(source, weights_ref, z, DELTA) + force_rows(force_ref, z, slot)
            if slot < M - 1:
                put(target, z, value)
            else:
                out_ref[z] = value
        source, target = target, source


def residual_kernel(place_ref, initial_ref, carried_ref, force_ref, fine_ref, coarse_ref, mine_ref, other_ref,
                    state_a, state_b, coarse_part):
    zones = fine_ref.shape[0]
    leading = place_ref[0] == 0
    second = place_ref[1] == 1
    for z in range(zones):
        put(state_a, z, jnp.where(leading, first_rows(initial_ref, z), carried_ref[z]))
    for z in range(zones):
        coarse_part[z] = propagate_zone(state_a, coarse_ref, z, DELTA * M)
    source, target = state_a, state_b
    for slot in range(M):
        for z in zone_order(zones, slot):
            value = propagate_zone(source, fine_ref, z, DELTA) + force_rows(force_ref, z, slot)
            if slot < M - 1:
                put(target, z, value)
            else:
                value = value - coarse_part[z]
                first, last = value[:8], value[8:]
                mine_ref[z] = jnp.where(second, last, first)
                other_ref[z] = jnp.where(second, first, last)
        source, target = target, source


def chain_kernel(turn, place_ref, incoming_ref, mine_ref, core_ref, side_ref, across_ref, coarse_ref, old_ref, out_ref,
                 state_a, state_b):
    zones = coarse_ref.shape[0]
    core, row, plane = place_ref[1], place_ref[2], place_ref[3]

    @pl.when(plane == turn)
    def _():
        for z in range(zones):
            value = incoming_ref[z]
            out_ref[0, z] = value
            put(state_a, z, value)
        source, target = state_a, state_b
        for step in range(M):
            here = row == step // 2
            own = core == step % 2
            for z in zone_order(zones, step):
                near = jnp.where(own, mine_ref[z], core_ref[z])
                far = jnp.where(own, side_ref[z], across_ref[z])
                value = propagate_zone(source, coarse_ref, z, DELTA * M) + jnp.where(here, near, far)
                out_ref[step + 1, z] = value
                if step < M - 1:
                    put(target, z, value)
            source, target = target, source


def final_kernel(place_ref, chain_ref, swapped_ref, force_ref, fine_ref, out_ref, state_a, state_b):
    zones = fine_ref.shape[0]
    per = out_ref.shape[0] // 2
    core, row = place_ref[1], place_ref[2]
    second = core == 1
    slot = row * 2 + core

    def both(index, zone):
        own, got = chain_ref[slot + index, zone], swapped_ref[index, zone]
        return jnp.concatenate([jnp.where(second, got, own), jnp.where(second, own, got)], axis=0)

    def write(zone, time, value):
        for i in range(2):
            out_ref[pl.ds(i * per + zone * M + time, 8, stride=zones * M), :] = value[i * 8:(i + 1) * 8]

    for z in range(zones):
        put(state_a, z, both(0, z))
        write(z, M - 1, both(1, z))
    source, target = state_a, state_b
    for step in range(M - 1):
        for z in zone_order(zones, step):
            value = propagate_zone(source, fine_ref, z, DELTA) + force_rows(force_ref, z, step)
            write(z, step, value)
            if step < M - 2:
                put(target, z, value)
        source, target = target, source


def states(zones, rows):
    return [pltpu.VMEM((zones + 2, 2 * rows, BLK), BF16)] * 2


def body(initial, forcing, fine_blocks, coarse_blocks):
    members, times, cells = forcing.shape
    blocks = cells // BLK
    zones = fine_blocks.shape[0]
    depth = blocks // zones
    index = lax.axis_index("tm")
    core, row, plane = index % 2, (index // 2) % 2, index // 4
    place = jnp.stack([index, core, row, plane]).astype(jnp.int32)
    count = lax.axis_size("tm")

    force = forcing.reshape(members, times, blocks, BLK).transpose(0, 2, 1, 3).reshape(members * blocks * times, BLK)
    start = initial.reshape(members, blocks, BLK).transpose(1, 0, 2).reshape(blocks * members, BLK)
    rows = members * depth

    fine = prepare(fine_blocks)
    corner = pl.pallas_call(
        relax_kernel,
        in_specs=[SMEM, VMEM, VMEM, VMEM],
        out_specs=VMEM,
        out_shape=jax.ShapeDtypeStruct((zones, rows, BLK), F32),
        scratch_shapes=states(zones, rows),
        cost_estimate=pl.CostEstimate(flops=10**9, bytes_accessed=10**6, transcendentals=0),
        name="relax",
    )(place, start, force, fine)
    carried = lax.ppermute(corner, "tm", [(i, i + 1) for i in range(count - 1)])
    coarse = prepare(coarse_blocks)
    half = jax.ShapeDtypeStruct((zones, depth, BLK), F32)
    mine, other = pl.pallas_call(
        residual_kernel,
        in_specs=[SMEM, VMEM, VMEM, VMEM, VMEM, VMEM],
        out_specs=[VMEM, VMEM],
        out_shape=[half, half],
        scratch_shapes=states(zones, rows) + [pltpu.VMEM((zones, rows, BLK), F32)],
        name="residual",
    )(place, start, carried, force, fine, coarse)
    from_core = lax.ppermute(other, "tm", [(i, i ^ 1) for i in range(count)])
    from_side = lax.ppermute(mine, "tm", [(i, i ^ 2) for i in range(count)])
    from_across = lax.ppermute(other, "tm", [(i, i ^ 3) for i in range(count)])

    incoming = lax.dynamic_index_in_dim(
        initial.reshape(members, depth, zones, BLK).transpose(0, 2, 1, 3), core, 0, keepdims=False
    )
    chain = jnp.zeros((M + 1, zones, depth, BLK), F32)
    planes = count // 4
    for turn in range(planes):
        chain = pl.pallas_call(
            functools.partial(chain_kernel, turn),
            in_specs=[SMEM] + [VMEM] * 7,
            out_specs=VMEM,
            out_shape=jax.ShapeDtypeStruct(chain.shape, F32),
            scratch_shapes=states(zones, depth),
            input_output_aliases={7: 0},
            name=f"chain{turn}",
        )(place, incoming, mine, from_core, from_side, from_across, coarse, chain)
        if turn < planes - 1:
            incoming = lax.ppermute(chain[M], "tm", [(turn * 4 + i, turn * 4 + 4 + i) for i in range(4)])
    give = lax.dynamic_slice_in_dim(chain, row * 2 + 1 - core, 2, 0)
    swapped = lax.ppermute(give, "tm", [(i, i ^ 1) for i in range(count)])
    result = pl.pallas_call(
        final_kernel,
        in_specs=[SMEM, VMEM, VMEM, VMEM, VMEM],
        out_specs=VMEM,
        out_shape=jax.ShapeDtypeStruct(force.shape, F32),
        scratch_shapes=states(zones, rows),
        name="final",
    )(place, chain, swapped, force, fine)
    return result.reshape(members, blocks, times, BLK).transpose(0, 2, 1, 3).reshape(members, times, cells)


def solution(mesh):
    in_specs = (P("grp", None), P("grp", "tm", None), P(), P())
    out_specs = P("grp", "tm", None)
    return jax.shard_map(body, mesh=mesh, in_specs=in_specs, out_specs=out_specs, check_vma=False)
```

```python
import functools

import jax
import jax.numpy as jnp
from jax import lax
from jax.experimental import pallas as pl
from jax.experimental.pallas import tpu as pltpu
from jax.sharding import PartitionSpec as P

M = 4
DELTA = 0.05
BLK = 128
BF16 = jnp.bfloat16
F32 = jnp.float32


def split(value):
    high = value.astype(BF16)
    low = (value - high.astype(F32)).astype(BF16)
    return jnp.concatenate([high, low], axis=0)


def shifted(value, down):
    parts = []
    for part in jnp.split(value, value.shape[0] // 8, axis=0):
        rows = lax.broadcasted_iota(jnp.int32, part.shape, 0)
        moved = pltpu.roll(part, 1 if down else 7, axis=0)
        parts.append(jnp.where(rows == (0 if down else 7), 0.0, moved))
    return jnp.concatenate(parts, axis=0)


def put(state_ref, zone, value):
    zones = state_ref.shape[0] - 2
    state_ref[zone + 1] = split(value)
    if zone == zones - 1:
        state_ref[0] = split(shifted(value, True))
    if zone == 0:
        state_ref[zones + 1] = split(shifted(value, False))


def solve(mixing, step):
    solved = mixing
    for _ in range(2):
        squared = solved * solved
        solved = (mixing + (2.0 * step * solved) * squared) / ((1.0 - step) + (3.0 * step) * squared)
    return solved


def propagate_zone(state_ref, weights_ref, zone, step):
    rows = state_ref.shape[1] // 2
    lhs = jnp.concatenate([state_ref[zone], state_ref[zone + 1], state_ref[zone + 2]], axis=1)
    product = jnp.dot(lhs, weights_ref[zone], preferred_element_type=F32)
    low, high = product[rows:], product[:rows]
    mixing = high[:, :BLK] + (high[:, BLK:] + (low[:, :BLK] + low[:, BLK:]))
    return solve(mixing, step)


def zone_order(zones, start):
    return [(start + i) % zones for i in range(zones)]


def prepare_zone(block_ref, out_ref, zone):
    for k in range(3):
        turned = block_ref[zone, k].T
        high = turned.astype(BF16)
        out_ref[zone, k * BLK:(k + 1) * BLK, :BLK] = high
        out_ref[zone, k * BLK:(k + 1) * BLK, BLK:] = (turned - high.astype(F32)).astype(BF16)


def prepare_kernel(blocks_ref, out_ref):
    for z in range(blocks_ref.shape[0]):
        prepare_zone(blocks_ref, out_ref, z)


def place():
    index = lax.axis_index("tm")
    return index, index & 1, (index >> 1) & 1, index >> 2


VMEM = pl.BlockSpec(memory_space=pltpu.VMEM)


def force_rows(force_ref, zone, slot):
    per = force_ref.shape[0] // 2
    zones = per // (M * 8)
    return jnp.concatenate(
        [force_ref[pl.ds(i * per + zone * M + slot, 8, stride=zones * M), :] for i in range(2)], axis=0
    )


def first_rows(initial_ref, zone):
    zones = initial_ref.shape[0] // 16
    return jnp.concatenate([initial_ref[pl.ds(zone * 2 + i, 8, stride=zones * 2), :] for i in range(2)], axis=0)


def relax_kernel(initial_ref, force_ref, blocks_ref, out_ref, weights_ref, state_a, state_b):
    zones = weights_ref.shape[0]
    leading = place()[0] == 0
    for z in range(zones):
        put(state_a, z, force_rows(force_ref, z, 0))
        prepare_zone(blocks_ref, weights_ref, z)

    @pl.when(leading)
    def _():
        for z in range(zones):
            put(state_b, z, first_rows(initial_ref, z))
        for z in range(zones):
            put(state_a, z, propagate_zone(state_b, weights_ref, z, DELTA) + force_rows(force_ref, z, 0))

    source, target = state_a, state_b
    for slot in range(1, M):
        for z in zone_order(zones, slot - 1):
            value = propagate_zone(source, weights_ref, z, DELTA) + force_rows(force_ref, z, slot)
            if slot < M - 1:
                put(target, z, value)
            else:
                out_ref[z] = value
        source, target = target, source


def residual_kernel(initial_ref, carried_ref, force_ref, fine_ref, coarse_ref, mine_ref, other_ref,
                    state_a, state_b, coarse_part):
    zones = fine_ref.shape[0]
    index, core, _, _ = place()
    leading, second = index == 0, core == 1
    for z in range(zones):
        put(state_a, z, jnp.where(leading, first_rows(initial_ref, z), carried_ref[z]))
    for z in range(zones):
        coarse_part[z] = jnp.where(leading, 0.0, propagate_zone(state_a, coarse_ref, z, DELTA * M))
    source, target = state_a, state_b
    for slot in range(M):
        for z in zone_order(zones, slot):
            value = propagate_zone(source, fine_ref, z, DELTA) + force_rows(force_ref, z, slot)
            if slot < M - 1:
                put(target, z, value)
            else:
                value = value - coarse_part[z]
                first, last = value[:8], value[8:]
                mine_ref[z] = jnp.where(second, last, first)
                other_ref[z] = jnp.where(second, first, last)
        source, target = target, source


def chain_kernel(turn, incoming_ref, mine_ref, core_ref, side_ref, across_ref, coarse_ref, *refs):
    next_ref, keep_ref, give_ref, state_a, state_b, held_ref = refs[-6:]
    zones = coarse_ref.shape[0]
    _, core, row, plane = place()

    @pl.when(plane == turn)
    def _():
        for z in range(zones):
            if turn == 0:
                first = first_rows(incoming_ref, z)
                value = jnp.where(core == 1, first[8:], first[:8])
            else:
                value = incoming_ref[z]
                put(state_a, z, value)
            held_ref[0, z] = value
        source, target = state_a, state_b
        for step in range(M):
            here = row == step // 2
            own = core == step % 2
            for z in zone_order(zones, step):
                near = jnp.where(own, mine_ref[z], core_ref[z])
                far = jnp.where(own, side_ref[z], across_ref[z])
                value = jnp.where(here, near, far)
                if turn > 0 or step > 0:
                    value = propagate_zone(source, coarse_ref, z, DELTA * M) + value
                held_ref[step + 1, z] = value
                if step < M - 1:
                    put(target, z, value)
                else:
                    next_ref[z] = value
            source, target = target, source
        slot = row * 2
        for i in range(2):
            keep_ref[i] = held_ref[slot + core + i]
            give_ref[i] = held_ref[slot + 1 - core + i]


def final_kernel(keep_ref, swapped_ref, force_ref, fine_ref, out_ref, state_a, state_b):
    zones = fine_ref.shape[0]
    per = out_ref.shape[0] // 2
    second = place()[1] == 1

    def both(index, zone):
        own, got = keep_ref[index, zone], swapped_ref[index, zone]
        return jnp.concatenate([jnp.where(second, got, own), jnp.where(second, own, got)], axis=0)

    def write(zone, time, value):
        for i in range(2):
            out_ref[pl.ds(i * per + zone * M + time, 8, stride=zones * M), :] = value[i * 8:(i + 1) * 8]

    for z in range(zones):
        put(state_a, z, both(0, z))
        write(z, M - 1, both(1, z))
    source, target = state_a, state_b
    for step in range(M - 1):
        for z in zone_order(zones, step):
            value = propagate_zone(source, fine_ref, z, DELTA) + force_rows(force_ref, z, step)
            write(z, step, value)
            if step < M - 2:
                put(target, z, value)
        source, target = target, source


def states(zones, rows):
    return [pltpu.VMEM((zones + 2, 2 * rows, BLK), BF16)] * 2


def call(kernel, name, in_specs, out_shape, scratch, mib, flops, aliases=None):
    return pl.pallas_call(
        kernel,
        in_specs=in_specs,
        out_specs=jax.tree.map(lambda _: VMEM, out_shape),
        out_shape=out_shape,
        scratch_shapes=scratch,
        input_output_aliases=aliases or {},
        compiler_params=pltpu.CompilerParams(vmem_limit_bytes=mib * 2**20),
        cost_estimate=pl.CostEstimate(flops=flops, bytes_accessed=10**6, transcendentals=0),
        name=name,
    )


def body(initial, forcing, fine_blocks, coarse_blocks):
    members, times, cells = forcing.shape
    blocks = cells // BLK
    zones = fine_blocks.shape[0]
    depth = blocks // zones
    rows = members * depth
    count = lax.axis_size("tm")

    force = forcing.reshape(members, times, blocks, BLK).transpose(0, 2, 1, 3).reshape(members * blocks * times, BLK)
    start = initial.reshape(members, blocks, BLK).transpose(1, 0, 2).reshape(blocks * members, BLK)
    weights = jax.ShapeDtypeStruct((zones, 3 * BLK, 2 * BLK), BF16)
    full = jax.ShapeDtypeStruct((zones, rows, BLK), F32)
    half = jax.ShapeDtypeStruct((zones, depth, BLK), F32)
    pair = jax.ShapeDtypeStruct((2, zones, depth, BLK), F32)

    corner, fine = call(
        relax_kernel, "relax", [VMEM] * 3, [full, weights], states(zones, rows), 12, 10**9
    )(start, force, fine_blocks)
    carried = lax.ppermute(corner, "tm", [(i, i + 1) for i in range(count - 1)])
    coarse = call(prepare_kernel, "prepare", [VMEM], weights, [], 8, 10**9)(coarse_blocks)
    mine, other = call(
        residual_kernel, "residual", [VMEM] * 5, [half, half],
        states(zones, rows) + [pltpu.VMEM((zones, rows, BLK), F32)], 14, 10**9,
    )(start, carried, force, fine, coarse)
    from_core = lax.ppermute(other, "tm", [(i, i ^ 1) for i in range(count)])
    from_side = lax.ppermute(mine, "tm", [(i, i ^ 2) for i in range(count)])
    from_across = lax.ppermute(other, "tm", [(i, i ^ 3) for i in range(count)])

    incoming, kept = start, ()
    for turn in range(count // 4):
        following, *kept = call(
            functools.partial(chain_kernel, turn), f"chain{turn}", [VMEM] * (6 + len(kept)), [half, pair, pair],
            states(zones, depth) + [pltpu.VMEM((M + 1, zones, depth, BLK), F32)], 8, 10**9,
            {6: 1, 7: 2} if kept else None,
        )(incoming, mine, from_core, from_side, from_across, coarse, *kept)
        if turn < count // 4 - 1:
            incoming = lax.ppermute(following, "tm", [(turn * 4 + i, turn * 4 + 4 + i) for i in range(4)])
    keep, give = kept
    swapped = lax.ppermute(give, "tm", [(i, i ^ 1) for i in range(count)])
    result = call(
        final_kernel, "final", [VMEM] * 4, jax.ShapeDtypeStruct(force.shape, F32), states(zones, rows), 10, 10**9
    )(keep, swapped, force, fine)
    return result.reshape(members, blocks, times, BLK).transpose(0, 2, 1, 3).reshape(members, times, cells)


def solution(mesh):
    in_specs = (P("grp", None), P("grp", "tm", None), P(), P())
    out_specs = P("grp", "tm", None)
    return jax.shard_map(body, mesh=mesh, in_specs=in_specs, out_specs=out_specs, check_vma=False)
```

```python
import functools

import jax
import jax.numpy as jnp
from jax import lax
from jax.experimental import pallas as pl
from jax.experimental.pallas import tpu as pltpu
from jax.sharding import PartitionSpec as P

M = 4
DELTA = 0.05
BLK = 128
BF16 = jnp.bfloat16
F32 = jnp.float32


def split(value):
    high = value.astype(BF16)
    low = (value - high.astype(F32)).astype(BF16)
    return jnp.concatenate([high, low], axis=0)


def shifted(value, down):
    parts = []
    for part in jnp.split(value, value.shape[0] // 8, axis=0):
        rows = lax.broadcasted_iota(jnp.int32, part.shape, 0)
        moved = pltpu.roll(part, 1 if down else 7, axis=0)
        parts.append(jnp.where(rows == (0 if down else 7), 0.0, moved))
    return jnp.concatenate(parts, axis=0)


def put(state_ref, zone, value):
    zones = state_ref.shape[0] - 2
    state_ref[zone + 1] = split(value)
    if zone == zones - 1:
        state_ref[0] = split(shifted(value, True))
    if zone == 0:
        state_ref[zones + 1] = split(shifted(value, False))


def solve(mixing, step):
    solved = mixing
    for _ in range(2):
        squared = solved * solved
        solved = (mixing + (2.0 * step * solved) * squared) / ((1.0 - step) + (3.0 * step) * squared)
    return solved


def propagate_zone(state_ref, weights_ref, zone, step):
    rows = state_ref.shape[1] // 2
    lhs = jnp.concatenate([state_ref[zone], state_ref[zone + 1], state_ref[zone + 2]], axis=1)
    product = jnp.dot(lhs, weights_ref[zone], preferred_element_type=F32)
    low, high = product[rows:], product[:rows]
    mixing = high[:, :BLK] + (high[:, BLK:] + (low[:, :BLK] + low[:, BLK:]))
    return solve(mixing, step)


def zone_order(zones, start):
    return [(start + i) % zones for i in range(zones)]


def prepare_zone(block_ref, out_ref, zone):
    for k in range(3):
        turned = block_ref[zone, k].T
        high = turned.astype(BF16)
        out_ref[zone, k * BLK:(k + 1) * BLK, :BLK] = high
        out_ref[zone, k * BLK:(k + 1) * BLK, BLK:] = (turned - high.astype(F32)).astype(BF16)


def fetches(blocks_ref, held_ref, sems):
    count = sems.shape[0]
    size = blocks_ref.shape[0] // count
    spans = [pl.ds(i * size, size) for i in range(count)]
    return [pltpu.make_async_copy(blocks_ref.at[s], held_ref.at[s], sems.at[i]) for i, s in enumerate(spans)]


def prepare_all(copies, held_ref, out_ref):
    size = held_ref.shape[0] // len(copies)
    for i, copy in enumerate(copies):
        copy.wait()
        for z in range(i * size, (i + 1) * size):
            prepare_zone(held_ref, out_ref, z)


def prepare_kernel(blocks_ref, out_ref, held_ref, sems):
    copies = fetches(blocks_ref, held_ref, sems)
    for copy in copies:
        copy.start()
    prepare_all(copies, held_ref, out_ref)


def place():
    index = lax.axis_index("tm")
    return index, index & 1, (index >> 1) & 1, index >> 2


VMEM = pl.BlockSpec(memory_space=pltpu.VMEM)


def force_rows(force_ref, zone, slot):
    per = force_ref.shape[0] // 2
    zones = per // (M * 8)
    return jnp.concatenate(
        [force_ref[pl.ds(i * per + zone * M + slot, 8, stride=zones * M), :] for i in range(2)], axis=0
    )


def first_rows(initial_ref, zone):
    zones = initial_ref.shape[0] // 16
    return jnp.concatenate([initial_ref[pl.ds(zone * 2 + i, 8, stride=zones * 2), :] for i in range(2)], axis=0)


def relax_kernel(initial_ref, force_ref, blocks_ref, out_ref, weights_ref, state_a, state_b, held_ref, sems):
    zones = weights_ref.shape[0]
    leading = place()[0] == 0
    copies = fetches(blocks_ref, held_ref, sems)
    for copy in copies:
        copy.start()
    for z in range(zones):
        put(state_a, z, force_rows(force_ref, z, 0))
    prepare_all(copies, held_ref, weights_ref)

    @pl.when(leading)
    def _():
        for z in range(zones):
            put(state_b, z, first_rows(initial_ref, z))
        for z in range(zones):
            put(state_a, z, propagate_zone(state_b, weights_ref, z, DELTA) + force_rows(force_ref, z, 0))

    source, target = state_a, state_b
    for slot in range(1, M):
        for z in zone_order(zones, slot - 1):
            value = propagate_zone(source, weights_ref, z, DELTA) + force_rows(force_ref, z, slot)
            if slot < M - 1:
                put(target, z, value)
            else:
                out_ref[z] = value
        source, target = target, source


def residual_kernel(initial_ref, carried_ref, force_ref, fine_ref, coarse_ref, out_ref, state_a, state_b, coarse_part):
    zones = fine_ref.shape[0]
    index = place()[0]
    for z in range(zones):
        put(state_a, z, jnp.where(index == 0, first_rows(initial_ref, z), carried_ref[z]))
    for z in range(zones):
        coarse_part[z] = jnp.where(index < 2, 0.0, propagate_zone(state_a, coarse_ref, z, DELTA * M))
    source, target = state_a, state_b
    for slot in range(M):
        for z in zone_order(zones, slot):
            value = propagate_zone(source, fine_ref, z, DELTA) + force_rows(force_ref, z, slot)
            if slot < M - 1:
                put(target, z, value)
            else:
                out_ref[z] = value - coarse_part[z]
        source, target = target, source


def chain_kernel(turn, incoming_ref, own_ref, core_ref, side_ref, far_ref, coarse_ref, *refs):
    next_ref, keep_ref, give_ref, state_a, state_b, held_ref = refs[-6:]
    zones = coarse_ref.shape[0]
    _, core, row, plane = place()
    begin = 2 if turn == 0 else 0

    @pl.when((plane == turn) & (core == 1))
    def _():
        def right(step, z):
            near, far = (own_ref, side_ref) if step % 2 else (core_ref, far_ref)
            return jnp.where(row == step // 2, near[z], far[z])

        for z in range(zones):
            held_ref[0, z] = first_rows(incoming_ref, z) if turn == 0 else incoming_ref[z]
            for step in range(begin):
                held_ref[step + 1, z] = right(step, z)
            put(state_a, z, held_ref[begin, z])
        source, target = state_a, state_b
        for step in range(begin, M):
            for z in zone_order(zones, step):
                value = propagate_zone(source, coarse_ref, z, DELTA * M) + right(step, z)
                held_ref[step + 1, z] = value
                if step < M - 1:
                    put(target, z, value)
                else:
                    next_ref[z] = value
            source, target = target, source
        for i in range(2):
            give_ref[i] = held_ref[row * 2 + i]
            keep_ref[i] = held_ref[row * 2 + 1 + i]


def final_kernel(keep_ref, swapped_ref, force_ref, fine_ref, out_ref, state_a, state_b):
    zones = fine_ref.shape[0]
    per = out_ref.shape[0] // 2
    keeps = place()[1] == 1

    def write(zone, time, value):
        for i in range(2):
            out_ref[pl.ds(i * per + zone * M + time, 8, stride=zones * M), :] = value[i * 8:(i + 1) * 8]

    for z in range(zones):
        put(state_a, z, jnp.where(keeps, keep_ref[0, z], swapped_ref[0, z]))
        write(z, M - 1, jnp.where(keeps, keep_ref[1, z], swapped_ref[1, z]))
    source, target = state_a, state_b
    for step in range(M - 1):
        for z in zone_order(zones, step):
            value = propagate_zone(source, fine_ref, z, DELTA) + force_rows(force_ref, z, step)
            write(z, step, value)
            if step < M - 2:
                put(target, z, value)
        source, target = target, source


def states(zones, rows):
    return [pltpu.VMEM((zones + 2, 2 * rows, BLK), BF16)] * 2


HBM = pl.BlockSpec(memory_space=pltpu.HBM)


def call(kernel, name, in_specs, out_shape, scratch, mib, flops, aliases=None):
    return pl.pallas_call(
        kernel,
        in_specs=in_specs,
        out_specs=jax.tree.map(lambda _: VMEM, out_shape),
        out_shape=out_shape,
        scratch_shapes=scratch,
        input_output_aliases=aliases or {},
        compiler_params=pltpu.CompilerParams(vmem_limit_bytes=mib * 2**20),
        cost_estimate=pl.CostEstimate(flops=flops, bytes_accessed=10**6, transcendentals=0),
        name=name,
    )


def body(initial, forcing, fine_blocks, coarse_blocks):
    members, times, cells = forcing.shape
    blocks = cells // BLK
    zones = fine_blocks.shape[0]
    depth = blocks // zones
    rows = members * depth
    count = lax.axis_size("tm")

    force = forcing.reshape(members, times, blocks, BLK).transpose(0, 2, 1, 3).reshape(members * blocks * times, BLK)
    start = initial.reshape(members, blocks, BLK).transpose(1, 0, 2).reshape(blocks * members, BLK)
    fine_blocks = pltpu.with_memory_space_constraint(fine_blocks, pltpu.HBM)
    coarse_blocks = pltpu.with_memory_space_constraint(coarse_blocks, pltpu.HBM)
    weights = jax.ShapeDtypeStruct((zones, 3 * BLK, 2 * BLK), BF16)
    full = jax.ShapeDtypeStruct((zones, rows, BLK), F32)
    pair = jax.ShapeDtypeStruct((2, zones, rows, BLK), F32)
    held = [pltpu.VMEM(fine_blocks.shape, F32), pltpu.SemaphoreType.DMA((8,))]

    def sent(value, even, odd):
        return lax.ppermute(value, "tm", [(i, (odd if i % 2 else even)(i) % count) for i in range(count)])

    corner, fine = call(
        relax_kernel, "relax", [VMEM, VMEM, HBM], [full, weights], states(zones, rows) + held, 16, 10**9
    )(start, force, fine_blocks)
    carried = sent(corner, lambda i: i + 1, lambda i: i + 1)
    coarse = call(prepare_kernel, "prepare", [HBM], weights, held, 12, 10**9)(coarse_blocks)
    right = call(
        residual_kernel, "residual", [VMEM] * 5, full,
        states(zones, rows) + [pltpu.VMEM((zones, rows, BLK), F32)], 14, 10**9,
    )(start, carried, force, fine, coarse)
    from_far = sent(right, lambda i: i ^ 3, lambda i: i ^ 1)
    from_side = sent(right, lambda i: i + 4, lambda i: i ^ 2)
    from_core = sent(right, lambda i: i ^ 1, lambda i: i ^ 1)

    incoming, kept = start, ()
    for turn in range(count // 4):
        following, *kept = call(
            functools.partial(chain_kernel, turn), f"chain{turn}", [VMEM] * (6 + len(kept)), [full, pair, pair],
            states(zones, rows) + [pltpu.VMEM((M + 1, zones, rows, BLK), F32)], 10, 10**9,
            {6: 1, 7: 2} if kept else None,
        )(incoming, right, from_core, from_side, from_far, coarse, *kept)
        if turn < count // 4 - 1:
            incoming = sent(following, lambda i: i ^ 2, lambda i: i + 4)
    keep, give = kept
    swapped = sent(give, lambda i: i ^ 1, lambda i: i ^ 1)
    result = call(
        final_kernel, "final", [VMEM] * 4, jax.ShapeDtypeStruct(force.shape, F32), states(zones, rows), 10, 10**9
    )(keep, swapped, force, fine)
    return result.reshape(members, blocks, times, BLK).transpose(0, 2, 1, 3).reshape(members, times, cells)


def solution(mesh):
    in_specs = (P("grp", None), P("grp", "tm", None), P(), P())
    out_specs = P("grp", "tm", None)
    return jax.shard_map(body, mesh=mesh, in_specs=in_specs, out_specs=out_specs, check_vma=False)
```

```python
import functools

import jax
import jax.numpy as jnp
from jax import lax
from jax.experimental import pallas as pl
from jax.experimental.pallas import tpu as pltpu
from jax.sharding import PartitionSpec as P

M = 4
DELTA = 0.05
BLK = 128
BF16 = jnp.bfloat16
F32 = jnp.float32


def split(value):
    high = value.astype(BF16)
    low = (value - high.astype(F32)).astype(BF16)
    return jnp.concatenate([high, low], axis=0)


def shifted(value, down):
    parts = []
    for part in jnp.split(value, value.shape[0] // 8, axis=0):
        rows = lax.broadcasted_iota(jnp.int32, part.shape, 0)
        moved = pltpu.roll(part, 1 if down else 7, axis=0)
        parts.append(jnp.where(rows == (0 if down else 7), 0.0, moved))
    return jnp.concatenate(parts, axis=0)


def put(state_ref, zone, value):
    zones = state_ref.shape[0] - 2
    state_ref[zone + 1] = split(value)
    if zone == zones - 1:
        state_ref[0] = split(shifted(value, True))
    if zone == 0:
        state_ref[zones + 1] = split(shifted(value, False))


def solve(mixing, step):
    solved = mixing
    for _ in range(2):
        squared = solved * solved
        solved = (mixing + (2.0 * step * solved) * squared) / ((1.0 - step) + (3.0 * step) * squared)
    return solved


def propagate_zone(state_ref, weights_ref, zone, step):
    rows = state_ref.shape[1] // 2
    lhs = jnp.concatenate([state_ref[zone], state_ref[zone + 1], state_ref[zone + 2]], axis=1)
    product = jnp.dot(lhs, weights_ref[zone], preferred_element_type=F32)
    low, high = product[rows:], product[:rows]
    mixing = high[:, :BLK] + (high[:, BLK:] + (low[:, :BLK] + low[:, BLK:]))
    return solve(mixing, step)


def zone_order(zones, start):
    return [(start + i) % zones for i in range(zones)]


def prepare_zone(block_ref, out_ref, zone):
    for k in range(3):
        turned = block_ref[zone, k].T
        high = turned.astype(BF16)
        out_ref[zone, k * BLK:(k + 1) * BLK, :BLK] = high
        out_ref[zone, k * BLK:(k + 1) * BLK, BLK:] = (turned - high.astype(F32)).astype(BF16)


def fetches(blocks_ref, held_ref, sems):
    count = sems.shape[0]
    size = blocks_ref.shape[0] // count
    spans = [pl.ds(i * size, size) for i in range(count)]
    return [pltpu.make_async_copy(blocks_ref.at[s], held_ref.at[s], sems.at[i]) for i, s in enumerate(spans)]


def prepare_all(copies, held_ref, out_ref):
    size = held_ref.shape[0] // len(copies)
    for i, copy in enumerate(copies):
        copy.wait()
        for z in range(i * size, (i + 1) * size):
            prepare_zone(held_ref, out_ref, z)


def prepare_kernel(blocks_ref, out_ref, held_ref, sems):
    copies = fetches(blocks_ref, held_ref, sems)
    for copy in copies:
        copy.start()
    prepare_all(copies, held_ref, out_ref)


def place():
    index = lax.axis_index("tm")
    return index, index & 1, (index >> 1) & 1, index >> 2


VMEM = pl.BlockSpec(memory_space=pltpu.VMEM)


def force_rows(force_ref, zone, slot):
    per = force_ref.shape[0] // 2
    zones = per // (M * 8)
    return jnp.concatenate(
        [force_ref[pl.ds(i * per + zone * M + slot, 8, stride=zones * M), :] for i in range(2)], axis=0
    )


def first_rows(initial_ref, zone):
    zones = initial_ref.shape[0] // 16
    return jnp.concatenate([initial_ref[pl.ds(zone * 2 + i, 8, stride=zones * 2), :] for i in range(2)], axis=0)


def relax_kernel(start_ref, given_ref, blocks_ref, out_ref, weights_ref, state_a, state_b, held_ref, sems,
                 initial_ref, force_ref, early_sems):
    zones = weights_ref.shape[0]
    leading = place()[0] == 0
    early = [
        pltpu.make_async_copy(given_ref, force_ref, early_sems.at[0]),
        pltpu.make_async_copy(start_ref, initial_ref, early_sems.at[1]),
    ]
    copies = fetches(blocks_ref, held_ref, sems)
    for copy in early + copies:
        copy.start()
    for copy in early:
        copy.wait()
    for z in range(zones):
        put(state_a, z, force_rows(force_ref, z, 0))
    prepare_all(copies, held_ref, weights_ref)

    @pl.when(leading)
    def _():
        for z in range(zones):
            put(state_b, z, first_rows(initial_ref, z))
        for z in range(zones):
            put(state_a, z, propagate_zone(state_b, weights_ref, z, DELTA) + force_rows(force_ref, z, 0))

    source, target = state_a, state_b
    for slot in range(1, M):
        for z in zone_order(zones, slot - 1):
            value = propagate_zone(source, weights_ref, z, DELTA) + force_rows(force_ref, z, slot)
            if slot < M - 1:
                put(target, z, value)
            else:
                out_ref[z] = value
        source, target = target, source


def residual_kernel(initial_ref, core_ref, chip_ref, force_ref, fine_ref, coarse_ref, out_ref,
                    state_a, state_b, coarse_part):
    zones = fine_ref.shape[0]
    index, core, _, _ = place()
    for z in range(zones):
        carried = jnp.where(core == 1, core_ref[z], chip_ref[z])
        put(state_a, z, jnp.where(index == 0, first_rows(initial_ref, z), carried))
    for z in range(zones):
        coarse_part[z] = jnp.where(index < 2, 0.0, propagate_zone(state_a, coarse_ref, z, DELTA * M))
    source, target = state_a, state_b
    for slot in range(M):
        for z in zone_order(zones, slot):
            value = propagate_zone(source, fine_ref, z, DELTA) + force_rows(force_ref, z, slot)
            if slot < M - 1:
                put(target, z, value)
            else:
                out_ref[z] = value - coarse_part[z]
        source, target = target, source


def chain_kernel(turn, last, incoming_ref, own_ref, core_ref, side_ref, far_ref, coarse_ref, *refs):
    keep_ref, give_ref, state_a, state_b, held_ref = refs[-5:]
    zones = coarse_ref.shape[0]
    _, core, row, plane = place()
    begin = 2 if turn == 0 else 0

    @pl.when((plane == turn) & (core == 1))
    def _():
        def right(step, z):
            near, far = (own_ref, side_ref) if step % 2 else (core_ref, far_ref)
            return jnp.where(row == step // 2, near[z], far[z])

        for z in range(zones):
            held_ref[0, z] = first_rows(incoming_ref, z) if turn == 0 else incoming_ref[z]
            for step in range(begin):
                held_ref[step + 1, z] = right(step, z)
            put(state_a, z, held_ref[begin, z])
        source, target = state_a, state_b
        for step in range(begin, M):
            for z in zone_order(zones, step):
                value = propagate_zone(source, coarse_ref, z, DELTA * M) + right(step, z)
                held_ref[step + 1, z] = value
                if step < M - 1:
                    put(target, z, value)
                elif not last:
                    refs[-6][z] = value
            source, target = target, source
        for i in range(2):
            give_ref[i] = held_ref[row * 2 + i]
            keep_ref[i] = held_ref[row * 2 + 1 + i]


def final_kernel(keep_ref, swapped_ref, force_ref, fine_ref, out_ref, state_a, state_b):
    zones = fine_ref.shape[0]
    per = out_ref.shape[0] // 2
    keeps = place()[1] == 1

    def write(zone, time, value):
        for i in range(2):
            out_ref[pl.ds(i * per + zone * M + time, 8, stride=zones * M), :] = value[i * 8:(i + 1) * 8]

    for z in range(zones):
        put(state_a, z, jnp.where(keeps, keep_ref[0, z], swapped_ref[0, z]))
        write(z, M - 1, jnp.where(keeps, keep_ref[1, z], swapped_ref[1, z]))
    source, target = state_a, state_b
    for step in range(M - 1):
        for z in zone_order(zones, step):
            value = propagate_zone(source, fine_ref, z, DELTA) + force_rows(force_ref, z, step)
            write(z, step, value)
            if step < M - 2:
                put(target, z, value)
        source, target = target, source


def states(zones, rows):
    return [pltpu.VMEM((zones + 2, 2 * rows, BLK), BF16)] * 2


HBM = pl.BlockSpec(memory_space=pltpu.HBM)


def call(kernel, name, in_specs, out_shape, scratch, mib, flops, aliases=None):
    return pl.pallas_call(
        kernel,
        in_specs=in_specs,
        out_specs=jax.tree.map(lambda _: VMEM, out_shape),
        out_shape=out_shape,
        scratch_shapes=scratch,
        input_output_aliases=aliases or {},
        compiler_params=pltpu.CompilerParams(vmem_limit_bytes=mib * 2**20),
        cost_estimate=pl.CostEstimate(flops=flops, bytes_accessed=10**6, transcendentals=0),
        name=name,
    )


def body(initial, forcing, fine_blocks, coarse_blocks):
    members, times, cells = forcing.shape
    blocks = cells // BLK
    zones = fine_blocks.shape[0]
    depth = blocks // zones
    rows = members * depth
    count = lax.axis_size("tm")

    force = forcing.reshape(members, times, blocks, BLK).transpose(0, 2, 1, 3).reshape(members * blocks * times, BLK)
    start = initial.reshape(members, blocks, BLK).transpose(1, 0, 2).reshape(blocks * members, BLK)
    fine_blocks = pltpu.with_memory_space_constraint(fine_blocks, pltpu.HBM)
    coarse_blocks = pltpu.with_memory_space_constraint(coarse_blocks, pltpu.HBM)
    weights = jax.ShapeDtypeStruct((zones, 3 * BLK, 2 * BLK), BF16)
    full = jax.ShapeDtypeStruct((zones, rows, BLK), F32)
    pair = jax.ShapeDtypeStruct((2, zones, rows, BLK), F32)
    held = [pltpu.VMEM(fine_blocks.shape, F32), pltpu.SemaphoreType.DMA((4,))]

    def sent(value, even, odd):
        return lax.ppermute(value, "tm", [(i, (odd if i % 2 else even)(i) % count) for i in range(count)])

    early = [pltpu.VMEM(start.shape, F32), pltpu.VMEM(force.shape, F32), pltpu.SemaphoreType.DMA((2,))]
    corner, fine = call(
        relax_kernel, "relax", [HBM] * 3, [full, weights], states(zones, rows) + held + early, 16, 10**9
    )(pltpu.with_memory_space_constraint(start, pltpu.HBM), pltpu.with_memory_space_constraint(force, pltpu.HBM),
      fine_blocks)
    across = {i: i + 1 for i in range(count - 1)}
    across[2], across[count - 1] = 0, 3
    from_chip = lax.ppermute(corner, "tm", list(across.items()))
    from_pair = sent(corner, lambda i: i ^ 1, lambda i: i ^ 1)
    coarse = call(prepare_kernel, "prepare", [HBM], weights, held, 12, 10**9)(coarse_blocks)
    right = call(
        residual_kernel, "residual", [VMEM] * 6, full,
        states(zones, rows) + [pltpu.VMEM((zones, rows, BLK), F32)], 14, 10**9,
    )(start, from_pair, from_chip, force, fine, coarse)
    from_side = sent(right, lambda i: i + 4, lambda i: i ^ 2)
    from_core = sent(right, lambda i: i ^ 1, lambda i: i ^ 1)
    from_far = sent(from_core, lambda i: i + 4, lambda i: i ^ 2)

    incoming, kept, turns = start, (), count // 4
    for turn in range(turns):
        last = turn == turns - 1
        aliases = {6 + i: i + (not last) for i in range(2)} if kept else None
        *following, keep, give = call(
            functools.partial(chain_kernel, turn, last), f"chain{turn}", [VMEM] * (6 + len(kept)),
            ([] if last else [full]) + [pair, pair],
            states(zones, rows) + [pltpu.VMEM((M + 1, zones, rows, BLK), F32)], 10, 10**9, aliases,
        )(incoming, right, from_core, from_side, from_far, coarse, *kept)
        kept = (keep, give)
        if not last:
            incoming = sent(following[0], lambda i: i ^ 2, lambda i: i + 4)
    swapped = sent(give, lambda i: i ^ 1, lambda i: i ^ 1)
    result = call(
        final_kernel, "final", [VMEM] * 4, jax.ShapeDtypeStruct(force.shape, F32), states(zones, rows), 10, 10**9
    )(keep, swapped, force, fine)
    return result.reshape(members, blocks, times, BLK).transpose(0, 2, 1, 3).reshape(members, times, cells)


def solution(mesh):
    in_specs = (P("grp", None), P("grp", "tm", None), P(), P())
    out_specs = P("grp", "tm", None)
    return jax.shard_map(body, mesh=mesh, in_specs=in_specs, out_specs=out_specs, check_vma=False)
```

```python
import functools

import jax
import jax.numpy as jnp
from jax import lax
from jax.experimental import pallas as pl
from jax.experimental.pallas import tpu as pltpu
from jax.sharding import PartitionSpec as P

M = 4
DELTA = 0.05
BLK = 128
BF16 = jnp.bfloat16
F32 = jnp.float32


def split(value):
    high = value.astype(BF16)
    low = (value - high.astype(F32)).astype(BF16)
    return jnp.concatenate([high, low], axis=0)


def shifted(value, down):
    parts = []
    for part in jnp.split(value, value.shape[0] // 8, axis=0):
        rows = lax.broadcasted_iota(jnp.int32, part.shape, 0)
        moved = pltpu.roll(part, 1 if down else 7, axis=0)
        parts.append(jnp.where(rows == (0 if down else 7), 0.0, moved))
    return jnp.concatenate(parts, axis=0)


def put(state_ref, zone, value):
    zones = state_ref.shape[0] - 2
    state_ref[zone + 1] = split(value)
    if zone == zones - 1:
        state_ref[0] = split(shifted(value, True))
    if zone == 0:
        state_ref[zones + 1] = split(shifted(value, False))


def solve(mixing, step):
    solved = mixing
    for _ in range(2):
        squared = solved * solved
        solved = (mixing + (2.0 * step * solved) * squared) / ((1.0 - step) + (3.0 * step) * squared)
    return solved


def propagate_zone(state_ref, weights_ref, zone, step):
    rows = state_ref.shape[1] // 2
    product = sum(
        jnp.dot(state_ref[zone + k], weights_ref[zone, k * BLK:(k + 1) * BLK], preferred_element_type=F32)
        for k in range(3)
    )
    low, high = product[rows:], product[:rows]
    mixing = high[:, :BLK] + (high[:, BLK:] + (low[:, :BLK] + low[:, BLK:]))
    return solve(mixing, step)


def zone_order(zones, start):
    return [(start + i) % zones for i in range(zones)]


def prepare_zone(block_ref, out_ref, zone):
    for k in range(3):
        turned = block_ref[zone, k].T
        high = turned.astype(BF16)
        out_ref[zone, k * BLK:(k + 1) * BLK, :BLK] = high
        out_ref[zone, k * BLK:(k + 1) * BLK, BLK:] = (turned - high.astype(F32)).astype(BF16)


def fetches(blocks_ref, held_ref, sems):
    count = sems.shape[0]
    size = blocks_ref.shape[0] // count
    spans = [pl.ds(i * size, size) for i in range(count)]
    return [pltpu.make_async_copy(blocks_ref.at[s], held_ref.at[s], sems.at[i]) for i, s in enumerate(spans)]


def prepare_all(copies, held_ref, out_ref):
    size = held_ref.shape[0] // len(copies)
    for i, copy in enumerate(copies):
        copy.wait()
        for z in range(i * size, (i + 1) * size):
            prepare_zone(held_ref, out_ref, z)


def prepare_kernel(blocks_ref, out_ref, held_ref, sems):
    copies = fetches(blocks_ref, held_ref, sems)
    for copy in copies:
        copy.start()
    prepare_all(copies, held_ref, out_ref)


def place():
    index = lax.axis_index("tm")
    return index, index & 1, (index >> 1) & 1, index >> 2


VMEM = pl.BlockSpec(memory_space=pltpu.VMEM)


def force_rows(force_ref, zone, slot):
    per = force_ref.shape[0] // 2
    zones = per // (M * 8)
    return jnp.concatenate(
        [force_ref[pl.ds(i * per + zone * M + slot, 8, stride=zones * M), :] for i in range(2)], axis=0
    )


def first_rows(initial_ref, zone):
    zones = initial_ref.shape[0] // 16
    return jnp.concatenate([initial_ref[pl.ds(zone * 2 + i, 8, stride=zones * 2), :] for i in range(2)], axis=0)


def relax_kernel(start_ref, given_ref, blocks_ref, out_ref, weights_ref, state_a, state_b, held_ref, sems,
                 initial_ref, force_ref, early_sems):
    zones = weights_ref.shape[0]
    leading = place()[0] == 0
    early = [
        pltpu.make_async_copy(given_ref, force_ref, early_sems.at[0]),
        pltpu.make_async_copy(start_ref, initial_ref, early_sems.at[1]),
    ]
    copies = fetches(blocks_ref, held_ref, sems)
    for copy in early + copies:
        copy.start()
    for copy in early:
        copy.wait()
    for z in range(zones):
        put(state_a, z, force_rows(force_ref, z, 0))
    prepare_all(copies, held_ref, weights_ref)

    @pl.when(leading)
    def _():
        for z in range(zones):
            put(state_b, z, first_rows(initial_ref, z))
        for z in range(zones):
            put(state_a, z, propagate_zone(state_b, weights_ref, z, DELTA) + force_rows(force_ref, z, 0))

    source, target = state_a, state_b
    for slot in range(1, M):
        for z in zone_order(zones, slot - 1):
            value = propagate_zone(source, weights_ref, z, DELTA) + force_rows(force_ref, z, slot)
            if slot < M - 1:
                put(target, z, value)
            else:
                out_ref[z] = value
        source, target = target, source


def residual_kernel(initial_ref, core_ref, chip_ref, force_ref, fine_ref, coarse_ref, out_ref,
                    state_a, state_b, coarse_part):
    zones = fine_ref.shape[0]
    index, core, _, _ = place()
    for z in range(zones):
        carried = jnp.where(core == 1, core_ref[z], chip_ref[z])
        put(state_a, z, jnp.where(index == 0, first_rows(initial_ref, z), carried))
    for z in range(zones):
        coarse_part[z] = jnp.where(index < 2, 0.0, propagate_zone(state_a, coarse_ref, z, DELTA * M))
    source, target = state_a, state_b
    for slot in range(M):
        for z in zone_order(zones, slot):
            value = propagate_zone(source, fine_ref, z, DELTA) + force_rows(force_ref, z, slot)
            if slot < M - 1:
                put(target, z, value)
            else:
                out_ref[z] = value - coarse_part[z]
        source, target = target, source


def chain_kernel(turn, begin, end, known, give, follow, incoming_ref, own_ref, core_ref, far_ref, side_ref, coarse_ref, *refs):
    *refs, state_a, state_b = refs
    old_ref = refs.pop(0) if turn > 0 or begin > known else None
    held_ref = refs.pop(0)
    zones = coarse_ref.shape[0]
    _, core, row, plane = place()

    @pl.when((plane == turn) & (core == 1))
    def _():
        def right(step, z):
            near, far = (own_ref, side_ref) if step % 2 else (core_ref, far_ref)
            return jnp.where(row == step // 2, near[z], far[z])

        for z in range(zones):
            if begin > known:
                put(state_a, z, old_ref[begin, z])
                continue
            held_ref[0, z] = first_rows(incoming_ref, z) if turn == 0 else incoming_ref[z]
            for step in range(known):
                held_ref[step + 1, z] = right(step, z)
            put(state_a, z, held_ref[known, z])
        source, target = state_a, state_b
        for step in range(begin, end):
            for z in zone_order(zones, step):
                value = propagate_zone(source, coarse_ref, z, DELTA * M) + right(step, z)
                held_ref[step + 1, z] = value
                if step < end - 1:
                    put(target, z, value)
                elif follow:
                    refs[0][z] = value
            source, target = target, source

    if give is not None:
        refs[-1][...] = held_ref[row * 2 + give]


def final_kernel(held_ref, swapped_ref, force_ref, fine_ref, out_ref, state_a, state_b):
    zones = fine_ref.shape[0]
    per = out_ref.shape[0] // 2
    _, core, row, _ = place()
    for z in range(zones):
        put(state_a, z, jnp.where(core == 1, held_ref[row * 2 + 1, z], swapped_ref[z]))
    source, target = state_a, state_b
    for step in range(M - 1):
        for z in zone_order(zones, step):
            value = propagate_zone(source, fine_ref, z, DELTA) + force_rows(force_ref, z, step)
            for i in range(2):
                out_ref[pl.ds(i * per + z * M + step, 8, stride=zones * M), :] = value[i * 8:(i + 1) * 8]
            if step < M - 2:
                put(target, z, value)
        source, target = target, source


def corners_kernel(steps_ref, held_ref, swapped_ref, out_ref):
    zones = swapped_ref.shape[0]
    per = out_ref.shape[0] // 2
    _, core, row, _ = place()
    out_ref[...] = steps_ref[...]
    for z in range(zones):
        value = jnp.where(core == 1, held_ref[row * 2 + 2, z], swapped_ref[z])
        for i in range(2):
            out_ref[pl.ds(i * per + z * M + M - 1, 8, stride=zones * M), :] = value[i * 8:(i + 1) * 8]


def states(zones, rows):
    return [pltpu.VMEM((zones + 2, 2 * rows, BLK), BF16)] * 2


HBM = pl.BlockSpec(memory_space=pltpu.HBM)


def call(kernel, name, in_specs, out_shape, scratch, mib, flops, aliases=None):
    return pl.pallas_call(
        kernel,
        in_specs=in_specs,
        out_specs=jax.tree.map(lambda _: VMEM, out_shape),
        out_shape=out_shape,
        scratch_shapes=scratch,
        input_output_aliases=aliases or {},
        compiler_params=pltpu.CompilerParams(vmem_limit_bytes=mib * 2**20),
        cost_estimate=pl.CostEstimate(flops=flops, bytes_accessed=10**6, transcendentals=0),
        name=name,
    )


def body(initial, forcing, fine_blocks, coarse_blocks):
    members, times, cells = forcing.shape
    blocks = cells // BLK
    zones = fine_blocks.shape[0]
    depth = blocks // zones
    rows = members * depth
    count = lax.axis_size("tm")

    force = forcing.reshape(members, times, blocks, BLK).transpose(0, 2, 1, 3).reshape(members * blocks * times, BLK)
    start = initial.reshape(members, blocks, BLK).transpose(1, 0, 2).reshape(blocks * members, BLK)
    fine_blocks = pltpu.with_memory_space_constraint(fine_blocks, pltpu.HBM)
    coarse_blocks = pltpu.with_memory_space_constraint(coarse_blocks, pltpu.HBM)
    weights = jax.ShapeDtypeStruct((zones, 3 * BLK, 2 * BLK), BF16)
    full = jax.ShapeDtypeStruct((zones, rows, BLK), F32)
    held_states = jax.ShapeDtypeStruct((M + 1, zones, rows, BLK), F32)
    held = [pltpu.VMEM(fine_blocks.shape, F32), pltpu.SemaphoreType.DMA((4,))]

    def sent(value, even, odd):
        return lax.ppermute(value, "tm", [(i, (odd if i % 2 else even)(i) % count) for i in range(count)])

    early = [pltpu.VMEM(start.shape, F32), pltpu.VMEM(force.shape, F32), pltpu.SemaphoreType.DMA((2,))]
    corner, fine = call(
        relax_kernel, "relax", [HBM] * 3, [full, weights], states(zones, rows) + held + early, 16, 10**9
    )(pltpu.with_memory_space_constraint(start, pltpu.HBM), pltpu.with_memory_space_constraint(force, pltpu.HBM),
      fine_blocks)
    across = {i: i + 1 for i in range(count - 1)}
    across[2], across[count - 1] = 0, 3
    from_chip = lax.ppermute(corner, "tm", list(across.items()))
    from_pair = sent(corner, lambda i: i ^ 1, lambda i: i ^ 1)
    coarse = call(prepare_kernel, "prepare", [HBM], weights, held, 12, 10**9)(coarse_blocks)
    right = call(
        residual_kernel, "residual", [VMEM] * 6, full,
        states(zones, rows) + [pltpu.VMEM((zones, rows, BLK), F32)], 14, 10**9,
    )(start, from_pair, from_chip, force, fine, coarse)
    from_side = lax.ppermute(right, "tm", [(i, i ^ 2) for i in range(1, count, 2)])
    from_far = sent(right, lambda i: i ^ 3, lambda i: i ^ 1)
    from_core = sent(right, lambda i: i ^ 1, lambda i: i ^ 1)

    def chain(turn, begin, end, known, give, follow, incoming, held):
        return call(
            functools.partial(chain_kernel, turn, begin, end, known, give, follow), f"chain{turn}_{end}",
            [VMEM] * (6 + len(held)), [held_states] + [full] * (follow + (give is not None)),
            states(zones, rows), 10, 10**9, {6: 0} if held else None,
        )(incoming, right, from_core, from_far, from_side, coarse, *held)

    incoming, held, turns = start, (), count // 4
    for turn in range(turns - 1):
        known = 2 if turn == 0 else 0
        *held, following = chain(turn, known, M, known, None, True, incoming, held)
        incoming = sent(following, lambda i: i ^ 2, lambda i: i + 4)
    *held, give = chain(turns - 1, 0, 2, 0, 0, False, incoming, held)
    swapped = sent(give, lambda i: i ^ 1, lambda i: i ^ 1)
    *held, give = chain(turns - 1, 2, M, 0, 1, False, incoming, held)
    corners = sent(give, lambda i: i ^ 1, lambda i: i ^ 1)
    forces = jax.ShapeDtypeStruct(force.shape, F32)
    steps = call(final_kernel, "final", [VMEM] * 4, forces, states(zones, rows), 10, 10**9)(*held, swapped, force, fine)
    result = call(corners_kernel, "corners", [VMEM] * 3, forces, [], 6, 10**6)(steps, *held, corners)
    return result.reshape(members, blocks, times, BLK).transpose(0, 2, 1, 3).reshape(members, times, cells)


def solution(mesh):
    in_specs = (P("grp", None), P("grp", "tm", None), P(), P())
    out_specs = P("grp", "tm", None)
    return jax.shard_map(body, mesh=mesh, in_specs=in_specs, out_specs=out_specs, check_vma=False)
```

```python
import functools

import jax
import jax.numpy as jnp
from jax import lax
from jax.experimental import pallas as pl
from jax.experimental.pallas import tpu as pltpu
from jax.sharding import PartitionSpec as P

M = 4
DELTA = 0.05
BLK = 128
BF16 = jnp.bfloat16
F32 = jnp.float32


def split(value):
    high = value.astype(BF16)
    low = (value - high.astype(F32)).astype(BF16)
    return jnp.concatenate([high, low], axis=0)


def shifted(value, down):
    parts = []
    for part in jnp.split(value, value.shape[0] // 8, axis=0):
        rows = lax.broadcasted_iota(jnp.int32, part.shape, 0)
        moved = pltpu.roll(part, 1 if down else 7, axis=0)
        parts.append(jnp.where(rows == (0 if down else 7), 0.0, moved))
    return jnp.concatenate(parts, axis=0)


def put(state_ref, zone, value):
    zones = state_ref.shape[0] - 2
    state_ref[zone + 1] = split(value)
    if zone == zones - 1:
        state_ref[0] = split(shifted(value, True))
    if zone == 0:
        state_ref[zones + 1] = split(shifted(value, False))


def solve(mixing, step):
    solved = mixing
    for _ in range(2):
        squared = solved * solved
        solved = (mixing + (2.0 * step * solved) * squared) / ((1.0 - step) + (3.0 * step) * squared)
    return solved


def propagate_zone(state_ref, weights_ref, zone, step):
    rows = state_ref.shape[1] // 2
    product = sum(
        jnp.dot(state_ref[zone + k], weights_ref[zone, k * BLK:(k + 1) * BLK], preferred_element_type=F32)
        for k in range(3)
    )
    low, high = product[rows:], product[:rows]
    mixing = high[:, :BLK] + (high[:, BLK:] + (low[:, :BLK] + low[:, BLK:]))
    return solve(mixing, step)


def zone_order(zones, start):
    return [(start + i) % zones for i in range(zones)]


def prepare_zone(block_ref, out_ref, zone):
    for k in range(3):
        turned = block_ref[zone, k].T
        high = turned.astype(BF16)
        out_ref[zone, k * BLK:(k + 1) * BLK, :BLK] = high
        out_ref[zone, k * BLK:(k + 1) * BLK, BLK:] = (turned - high.astype(F32)).astype(BF16)


def fetches(blocks_ref, held_ref, sems):
    count = sems.shape[0]
    size = blocks_ref.shape[0] // count
    spans = [pl.ds(i * size, size) for i in range(count)]
    return [pltpu.make_async_copy(blocks_ref.at[s], held_ref.at[s], sems.at[i]) for i, s in enumerate(spans)]


def prepare_all(copies, held_ref, out_ref):
    size = held_ref.shape[0] // len(copies)
    for i, copy in enumerate(copies):
        copy.wait()
        for z in range(i * size, (i + 1) * size):
            prepare_zone(held_ref, out_ref, z)


def prepare_kernel(blocks_ref, out_ref, held_ref, sems):
    copies = fetches(blocks_ref, held_ref, sems)
    for copy in copies:
        copy.start()
    prepare_all(copies, held_ref, out_ref)


def place():
    index = lax.axis_index("tm")
    return index, index & 1, (index >> 1) & 1, index >> 2


VMEM = pl.BlockSpec(memory_space=pltpu.VMEM)


def force_rows(force_ref, zone, slot):
    per = force_ref.shape[0] // 2
    zones = per // (M * 8)
    return jnp.concatenate(
        [force_ref[pl.ds(i * per + zone * M + slot, 8, stride=zones * M), :] for i in range(2)], axis=0
    )


def first_rows(initial_ref, zone):
    zones = initial_ref.shape[0] // 16
    return jnp.concatenate([initial_ref[pl.ds(zone * 2 + i, 8, stride=zones * 2), :] for i in range(2)], axis=0)


def relax_kernel(start_ref, given_ref, blocks_ref, out_ref, weights_ref, state_a, state_b, held_ref, sems,
                 initial_ref, force_ref, early_sems):
    zones = weights_ref.shape[0]
    leading = place()[0] == 0
    early = [
        pltpu.make_async_copy(given_ref, force_ref, early_sems.at[0]),
        pltpu.make_async_copy(start_ref, initial_ref, early_sems.at[1]),
    ]
    copies = fetches(blocks_ref, held_ref, sems)
    for copy in early + copies:
        copy.start()
    for copy in early:
        copy.wait()
    for z in range(zones):
        put(state_a, z, force_rows(force_ref, z, 0))
    prepare_all(copies, held_ref, weights_ref)

    @pl.when(leading)
    def _():
        for z in range(zones):
            put(state_b, z, first_rows(initial_ref, z))
        for z in range(zones):
            put(state_a, z, propagate_zone(state_b, weights_ref, z, DELTA) + force_rows(force_ref, z, 0))

    source, target = state_a, state_b
    for slot in range(1, M):
        for z in zone_order(zones, slot - 1):
            value = propagate_zone(source, weights_ref, z, DELTA) + force_rows(force_ref, z, slot)
            if slot < M - 1:
                put(target, z, value)
            else:
                out_ref[z] = value
        source, target = target, source


def residual_kernel(initial_ref, core_ref, chip_ref, force_ref, fine_ref, coarse_ref, out_ref,
                    state_a, state_b, coarse_part):
    zones = fine_ref.shape[0]
    index, core, _, _ = place()
    for z in range(zones):
        carried = jnp.where(core == 1, core_ref[z], chip_ref[z])
        put(state_a, z, jnp.where(index == 0, first_rows(initial_ref, z), carried))
    for z in range(zones):
        coarse_part[z] = jnp.where(index < 2, 0.0, propagate_zone(state_a, coarse_ref, z, DELTA * M))
    source, target = state_a, state_b
    for slot in range(M):
        for z in zone_order(zones, slot):
            value = propagate_zone(source, fine_ref, z, DELTA) + force_rows(force_ref, z, slot)
            if slot < M - 1:
                put(target, z, value)
            else:
                out_ref[z] = value - coarse_part[z]
        source, target = target, source


def march(source, target, coarse_ref, held_ref, rights, slot, done=None):
    zones = coarse_ref.shape[0]
    for step, right in enumerate(rights):
        for z in zone_order(zones, step):
            value = propagate_zone(source, coarse_ref, z, DELTA * M) + right(z)
            held_ref[slot + step + 1, z] = value
            if step < len(rights) - 1:
                put(target, z, value)
            elif done is not None:
                done[z] = value
        source, target = target, source


def first_chain_kernel(initial_ref, own_ref, down_ref, up_ref, coarse_ref, held_ref, next_ref, state_a, state_b):
    zones = coarse_ref.shape[0]
    _, core, row, plane = place()

    @pl.when((plane == 0) & (core == 1) & (row == 0))
    def _():
        for z in range(zones):
            held_ref[0, z] = first_rows(initial_ref, z)
            held_ref[1, z] = down_ref[z]
            held_ref[2, z] = own_ref[z]

    @pl.when((plane == 0) & (core == 1) & (row == 1))
    def _():
        for z in range(zones):
            held_ref[2, z] = down_ref[z]
            put(state_a, z, down_ref[z])
        march(state_a, state_b, coarse_ref, held_ref, [lambda z: up_ref[z], lambda z: own_ref[z]], 2, next_ref)


def chain_kernel(turn, incoming_refs, own_ref, down_ref, up_ref, far_ref, coarse_ref, held_ref, next_ref, state_a, state_b):
    zones = coarse_ref.shape[0]
    _, core, row, plane = place()
    upper = row == 0
    rights = [
        lambda z: jnp.where(upper, down_ref[z], far_ref[z]),
        lambda z: jnp.where(upper, own_ref[z], down_ref[z]),
        lambda z: jnp.where(upper, far_ref[z], up_ref[z]),
        lambda z: jnp.where(upper, up_ref[z], own_ref[z]),
    ]

    @pl.when((plane == turn) & (core == 1))
    def _():
        for z in range(zones):
            held_ref[0, z] = arrived(incoming_refs, upper, z)
            put(state_a, z, held_ref[0, z])
        march(state_a, state_b, coarse_ref, held_ref, rights, 0, next_ref)


def arrived(incoming_refs, upper, zone):
    if len(incoming_refs) == 1:
        return incoming_refs[0][zone]
    return jnp.where(upper, incoming_refs[0][zone], incoming_refs[1][zone])


def enter_kernel(turn, incoming_ref, own_ref, down_ref, up_ref, far_ref, coarse_ref, old_ref, held_ref, give_ref,
                 state_a, state_b):
    del own_ref, up_ref, old_ref
    zones = coarse_ref.shape[0]
    _, core, row, plane = place()
    here = (plane == turn) & (core == 1)

    @pl.when(here & (row == 0))
    def _():
        held_ref[0] = incoming_ref[...]

    @pl.when(here & (row == 1))
    def _():
        for z in range(zones):
            put(state_a, z, incoming_ref[z])
        march(state_a, state_b, coarse_ref, held_ref, [lambda z: far_ref[z], lambda z: down_ref[z]], 0)

    give_ref[...] = held_ref[row * 2]


def leave_kernel(turn, own_ref, down_ref, up_ref, coarse_ref, old_ref, held_ref, give_ref, state_a, state_b):
    zones = coarse_ref.shape[0]
    _, core, row, plane = place()

    @pl.when((plane == turn) & (core == 1))
    def _():
        for z in range(zones):
            put(state_a, z, old_ref[row * 2, z])
        near = lambda z: jnp.where(row == 0, down_ref[z], up_ref[z])
        march(state_a, state_b, coarse_ref, held_ref, [near, lambda z: own_ref[z]], row * 2)

    give_ref[...] = held_ref[row * 2 + 1]


def final_kernel(held_ref, swapped_ref, force_ref, fine_ref, out_ref, state_a, state_b):
    zones = fine_ref.shape[0]
    per = out_ref.shape[0] // 2
    _, core, row, _ = place()
    for z in range(zones):
        put(state_a, z, jnp.where(core == 1, held_ref[row * 2 + 1, z], swapped_ref[z]))
    source, target = state_a, state_b
    for step in range(M - 1):
        for z in zone_order(zones, step):
            value = propagate_zone(source, fine_ref, z, DELTA) + force_rows(force_ref, z, step)
            for i in range(2):
                out_ref[pl.ds(i * per + z * M + step, 8, stride=zones * M), :] = value[i * 8:(i + 1) * 8]
            if step < M - 2:
                put(target, z, value)
        source, target = target, source


def corners_kernel(steps_ref, held_ref, swapped_ref, out_ref):
    zones = swapped_ref.shape[0]
    per = out_ref.shape[0] // 2
    _, core, row, _ = place()
    out_ref[...] = steps_ref[...]
    for z in range(zones):
        value = jnp.where(core == 1, held_ref[row * 2 + 2, z], swapped_ref[z])
        for i in range(2):
            out_ref[pl.ds(i * per + z * M + M - 1, 8, stride=zones * M), :] = value[i * 8:(i + 1) * 8]


def states(zones, rows):
    return [pltpu.VMEM((zones + 2, 2 * rows, BLK), BF16)] * 2


HBM = pl.BlockSpec(memory_space=pltpu.HBM)


def call(kernel, name, in_specs, out_shape, scratch, mib, flops, aliases=None):
    return pl.pallas_call(
        kernel,
        in_specs=in_specs,
        out_specs=jax.tree.map(lambda _: VMEM, out_shape),
        out_shape=out_shape,
        scratch_shapes=scratch,
        input_output_aliases=aliases or {},
        compiler_params=pltpu.CompilerParams(vmem_limit_bytes=mib * 2**20),
        cost_estimate=pl.CostEstimate(flops=flops, bytes_accessed=10**6, transcendentals=0),
        name=name,
    )


def body(initial, forcing, fine_blocks, coarse_blocks):
    members, times, cells = forcing.shape
    blocks = cells // BLK
    zones = fine_blocks.shape[0]
    depth = blocks // zones
    rows = members * depth
    count = lax.axis_size("tm")

    force = forcing.reshape(members, times, blocks, BLK).transpose(0, 2, 1, 3).reshape(members * blocks * times, BLK)
    start = initial.reshape(members, blocks, BLK).transpose(1, 0, 2).reshape(blocks * members, BLK)
    fine_blocks = pltpu.with_memory_space_constraint(fine_blocks, pltpu.HBM)
    coarse_blocks = pltpu.with_memory_space_constraint(coarse_blocks, pltpu.HBM)
    weights = jax.ShapeDtypeStruct((zones, 3 * BLK, 2 * BLK), BF16)
    full = jax.ShapeDtypeStruct((zones, rows, BLK), F32)
    held_states = jax.ShapeDtypeStruct((M + 1, zones, rows, BLK), F32)
    held = [pltpu.VMEM(fine_blocks.shape, F32), pltpu.SemaphoreType.DMA((4,))]

    def sent(value, even, odd):
        return lax.ppermute(value, "tm", [(i, (odd if i % 2 else even)(i) % count) for i in range(count)])

    early = [pltpu.VMEM(start.shape, F32), pltpu.VMEM(force.shape, F32), pltpu.SemaphoreType.DMA((2,))]
    corner, fine = call(
        relax_kernel, "relax", [HBM] * 3, [full, weights], states(zones, rows) + held + early, 16, 10**9
    )(pltpu.with_memory_space_constraint(start, pltpu.HBM), pltpu.with_memory_space_constraint(force, pltpu.HBM),
      fine_blocks)
    across = {i: i + 1 for i in range(count - 1)}
    across[2], across[count - 1] = 0, 3
    from_chip = lax.ppermute(corner, "tm", list(across.items()))
    from_pair = sent(corner, lambda i: i ^ 1, lambda i: i ^ 1)
    coarse = call(prepare_kernel, "prepare", [HBM], weights, held, 12, 10**9)(coarse_blocks)
    right = call(
        residual_kernel, "residual", [VMEM] * 6, full,
        states(zones, rows) + [pltpu.VMEM((zones, rows, BLK), F32)], 14, 10**9,
    )(start, from_pair, from_chip, force, fine, coarse)
    def relayed(value, moves):
        target = {i: i ^ 1 for i in range(count)}
        for a, b in moves:
            target.update({2 * a + 1: 2 * b + 1, 2 * b + 1: 2 * b, 2 * b: 2 * a, 2 * a: 2 * a + 1})
        return lax.ppermute(value, "tm", list(target.items()))

    planes = range(count // 4)
    down = relayed(right, [(2 * p, 2 * p + 1) for p in planes])
    up = relayed(right, [(2 * p + 1, 2 * p) for p in planes])
    far = sent(right, lambda i: i ^ 3, lambda i: i ^ 1)

    def chain(kernel, name, inputs, outputs, held=None):
        return call(
            kernel, name, [VMEM] * (len(inputs) + (held is not None)), [held_states] + [full] * outputs,
            states(zones, rows), 10, 10**9, None if held is None else {len(inputs): 0},
        )(*inputs, *(() if held is None else (held,)))

    def middle(turn, arrivals):
        def kernel(*refs):
            incoming_refs, rest = refs[:arrivals], refs[arrivals:]
            chain_kernel(turn, incoming_refs, *rest[:5], *rest[6:])

        return kernel

    held, following = chain(first_chain_kernel, "chain0", (start, right, down, up, coarse), 1)
    incoming = (relayed(following, [(1, 2)]), relayed(following, [(1, 3)]))
    last = count // 4 - 1
    for turn in range(1, last):
        held, following = chain(
            middle(turn, len(incoming)), f"chain{turn}", (*incoming, right, down, up, far, coarse), 1, held)
        incoming = (relayed(following, [(2 * turn + y, 2 * turn + 2 + y) for y in range(2)]),)
    held, give = chain(
        functools.partial(enter_kernel, last), "enter", (*incoming, right, down, up, far, coarse), 1, held)
    swapped = sent(give, lambda i: i ^ 1, lambda i: i ^ 1)
    held, give = chain(functools.partial(leave_kernel, last), "leave", (right, down, up, coarse), 1, held)
    corners = sent(give, lambda i: i ^ 1, lambda i: i ^ 1)
    forces = jax.ShapeDtypeStruct(force.shape, F32)
    steps = call(final_kernel, "final", [VMEM] * 4, forces, states(zones, rows), 10, 10**9)(held, swapped, force, fine)
    result = call(corners_kernel, "corners", [VMEM] * 3, forces, [], 6, 10**6)(steps, held, corners)
    return result.reshape(members, blocks, times, BLK).transpose(0, 2, 1, 3).reshape(members, times, cells)


def solution(mesh):
    in_specs = (P("grp", None), P("grp", "tm", None), P(), P())
    out_specs = P("grp", "tm", None)
    return jax.shard_map(body, mesh=mesh, in_specs=in_specs, out_specs=out_specs, check_vma=False)
```

```python
import functools

import jax
import jax.numpy as jnp
from jax import lax
from jax.experimental import pallas as pl
from jax.experimental.pallas import tpu as pltpu
from jax.sharding import PartitionSpec as P

M = 4
DELTA = 0.05
BLK = 128
BF16 = jnp.bfloat16
F32 = jnp.float32


def split(value):
    high = value.astype(BF16)
    low = (value - high.astype(F32)).astype(BF16)
    return jnp.concatenate([high, low], axis=0)


def shifted(value, down):
    parts = []
    for part in jnp.split(value, value.shape[0] // 8, axis=0):
        rows = lax.broadcasted_iota(jnp.int32, part.shape, 0)
        moved = pltpu.roll(part, 1 if down else 7, axis=0)
        parts.append(jnp.where(rows == (0 if down else 7), 0.0, moved))
    return jnp.concatenate(parts, axis=0)


def put(state_ref, zone, value):
    zones = state_ref.shape[0] - 2
    state_ref[zone + 1] = split(value)
    if zone == zones - 1:
        state_ref[0] = split(shifted(value, True))
    if zone == 0:
        state_ref[zones + 1] = split(shifted(value, False))


def solve(mixing, step):
    solved = mixing
    for _ in range(2):
        squared = solved * solved
        solved = (mixing + (2.0 * step * solved) * squared) / ((1.0 - step) + (3.0 * step) * squared)
    return solved


def propagate_zone(state_ref, weights_ref, zone, step):
    rows = state_ref.shape[1] // 2
    product = sum(
        jnp.dot(state_ref[zone + k], weights_ref[zone, k * BLK:(k + 1) * BLK], preferred_element_type=F32)
        for k in range(3)
    )
    low, high = product[rows:], product[:rows]
    mixing = high[:, :BLK] + (high[:, BLK:] + (low[:, :BLK] + low[:, BLK:]))
    return solve(mixing, step)


def zone_order(zones, start):
    return [(start + i) % zones for i in range(zones)]


def prepare_zone(block_ref, out_ref, zone):
    for k in range(3):
        turned = block_ref[zone, k].T
        high = turned.astype(BF16)
        out_ref[zone, k * BLK:(k + 1) * BLK, :BLK] = high
        out_ref[zone, k * BLK:(k + 1) * BLK, BLK:] = (turned - high.astype(F32)).astype(BF16)


def fetches(blocks_ref, held_ref, sems):
    count = sems.shape[0]
    size = blocks_ref.shape[0] // count
    spans = [pl.ds(i * size, size) for i in range(count)]
    return [pltpu.make_async_copy(blocks_ref.at[s], held_ref.at[s], sems.at[i]) for i, s in enumerate(spans)]


def prepare_all(copies, held_ref, out_ref):
    size = held_ref.shape[0] // len(copies)
    for i, copy in enumerate(copies):
        copy.wait()
        for z in range(i * size, (i + 1) * size):
            prepare_zone(held_ref, out_ref, z)


def prepare_kernel(blocks_ref, out_ref):
    for z in range(blocks_ref.shape[0]):
        prepare_zone(blocks_ref, out_ref, z)


def place():
    index = lax.axis_index("tm")
    return index, index & 1, (index >> 1) & 1, index >> 2


VMEM = pl.BlockSpec(memory_space=pltpu.VMEM)


def force_rows(force_ref, zone, slot):
    per = force_ref.shape[0] // 2
    zones = per // (M * 8)
    return jnp.concatenate(
        [force_ref[pl.ds(i * per + zone * M + slot, 8, stride=zones * M), :] for i in range(2)], axis=0
    )


def first_rows(initial_ref, zone):
    zones = initial_ref.shape[0] // 16
    return jnp.concatenate([initial_ref[pl.ds(zone * 2 + i, 8, stride=zones * 2), :] for i in range(2)], axis=0)


def relax_kernel(start_ref, given_ref, blocks_ref, next_blocks_ref, out_ref, weights_ref, next_held_ref,
                 state_a, state_b, held_ref, sems, initial_ref, force_ref, early_sems, late_sems):
    zones = weights_ref.shape[0]
    leading = place()[0] == 0
    early = [
        pltpu.make_async_copy(given_ref, force_ref, early_sems.at[0]),
        pltpu.make_async_copy(start_ref, initial_ref, early_sems.at[1]),
    ]
    copies = fetches(blocks_ref, held_ref, sems)
    for copy in early + copies:
        copy.start()
    for copy in early:
        copy.wait()
    for z in range(zones):
        put(state_a, z, force_rows(force_ref, z, 0))
    prepare_all(copies, held_ref, weights_ref)
    late = fetches(next_blocks_ref, next_held_ref, late_sems)
    for copy in late:
        copy.start()

    @pl.when(leading)
    def _():
        for z in range(zones):
            put(state_b, z, first_rows(initial_ref, z))
        for z in range(zones):
            put(state_a, z, propagate_zone(state_b, weights_ref, z, DELTA) + force_rows(force_ref, z, 0))

    source, target = state_a, state_b
    for slot in range(1, M):
        for z in zone_order(zones, slot - 1):
            value = propagate_zone(source, weights_ref, z, DELTA) + force_rows(force_ref, z, slot)
            if slot < M - 1:
                put(target, z, value)
            else:
                out_ref[z] = value
        source, target = target, source
    for copy in late:
        copy.wait()


def residual_kernel(initial_ref, core_ref, chip_ref, force_ref, fine_ref, coarse_ref, out_ref,
                    state_a, state_b, coarse_part):
    zones = fine_ref.shape[0]
    index, core, _, _ = place()
    for z in range(zones):
        carried = jnp.where(core == 1, core_ref[z], chip_ref[z])
        put(state_a, z, jnp.where(index == 0, first_rows(initial_ref, z), carried))
    for z in range(zones):
        coarse_part[z] = jnp.where(index < 2, 0.0, propagate_zone(state_a, coarse_ref, z, DELTA * M))
    source, target = state_a, state_b
    for slot in range(M):
        for z in zone_order(zones, slot):
            value = propagate_zone(source, fine_ref, z, DELTA) + force_rows(force_ref, z, slot)
            if slot < M - 1:
                put(target, z, value)
            else:
                out_ref[z] = value - coarse_part[z]
        source, target = target, source


def march(source, target, coarse_ref, held_ref, rights, slot, done=None):
    zones = coarse_ref.shape[0]
    for step, right in enumerate(rights):
        for z in zone_order(zones, step):
            value = propagate_zone(source, coarse_ref, z, DELTA * M) + right(z)
            held_ref[slot + step + 1, z] = value
            if step < len(rights) - 1:
                put(target, z, value)
            elif done is not None:
                done[z] = value
        source, target = target, source


def first_chain_kernel(initial_ref, own_ref, pair_ref, up_ref, down_ref, coarse_ref, held_ref, next_ref, state_a, state_b):
    zones = coarse_ref.shape[0]
    _, core, row, plane = place()

    @pl.when((plane == 0) & (core == 1) & (row == 0))
    def _():
        for z in range(zones):
            held_ref[0, z] = first_rows(initial_ref, z)
            held_ref[1, z] = pair_ref[z]
            held_ref[2, z] = own_ref[z]

    @pl.when((plane == 0) & (core == 1) & (row == 1))
    def _():
        for z in range(zones):
            held_ref[2, z] = down_ref[z]
            put(state_a, z, down_ref[z])
        march(state_a, state_b, coarse_ref, held_ref, [lambda z: up_ref[z], lambda z: own_ref[z]], 2, next_ref)


def chain_kernel(turn, incoming_refs, own_ref, near_ref, far_ref, up_ref, down_ref, coarse_ref, held_ref, next_ref,
                 state_a, state_b):
    zones = coarse_ref.shape[0]
    _, core, row, plane = place()
    upper = row == 0
    rights = [
        lambda z: jnp.where(upper, near_ref[z], far_ref[z]),
        lambda z: jnp.where(upper, own_ref[z], down_ref[z]),
        lambda z: jnp.where(upper, down_ref[z], up_ref[z]),
        lambda z: jnp.where(upper, up_ref[z], own_ref[z]),
    ]

    @pl.when((plane == turn) & (core == 1))
    def _():
        for z in range(zones):
            held_ref[0, z] = arrived(incoming_refs, upper, z)
            put(state_a, z, held_ref[0, z])
        march(state_a, state_b, coarse_ref, held_ref, rights, 0, next_ref)


def arrived(incoming_refs, upper, zone):
    if len(incoming_refs) == 1:
        return incoming_refs[0][zone]
    return jnp.where(upper, incoming_refs[0][zone], incoming_refs[1][zone])


def enter_kernel(turn, incoming_ref, far_ref, down_ref, coarse_ref, old_ref, held_ref, give_ref, state_a, state_b):
    del old_ref
    zones = coarse_ref.shape[0]
    _, core, row, plane = place()
    here = (plane == turn) & (core == 1)

    @pl.when(here & (row == 0))
    def _():
        held_ref[0] = incoming_ref[...]

    @pl.when(here & (row == 1))
    def _():
        for z in range(zones):
            put(state_a, z, incoming_ref[z])
        march(state_a, state_b, coarse_ref, held_ref, [lambda z: far_ref[z], lambda z: down_ref[z]], 0)

    give_ref[...] = held_ref[row * 2]


def leave_kernel(turn, own_ref, near_ref, up_ref, coarse_ref, old_ref, held_ref, give_ref, state_a, state_b):
    zones = coarse_ref.shape[0]
    _, core, row, plane = place()

    @pl.when((plane == turn) & (core == 1))
    def _():
        for z in range(zones):
            put(state_a, z, old_ref[row * 2, z])
        near = lambda z: jnp.where(row == 0, near_ref[z], up_ref[z])
        march(state_a, state_b, coarse_ref, held_ref, [near, lambda z: own_ref[z]], row * 2)

    give_ref[...] = held_ref[row * 2 + 1]


def final_kernel(held_ref, swapped_ref, force_ref, fine_ref, out_ref, state_a, state_b):
    zones = fine_ref.shape[0]
    per = out_ref.shape[0] // 2
    _, core, row, _ = place()
    for z in range(zones):
        put(state_a, z, jnp.where(core == 1, held_ref[row * 2 + 1, z], swapped_ref[z]))
    source, target = state_a, state_b
    for step in range(M - 1):
        for z in zone_order(zones, step):
            value = propagate_zone(source, fine_ref, z, DELTA) + force_rows(force_ref, z, step)
            for i in range(2):
                out_ref[pl.ds(i * per + z * M + step, 8, stride=zones * M), :] = value[i * 8:(i + 1) * 8]
            if step < M - 2:
                put(target, z, value)
        source, target = target, source


def corners_kernel(steps_ref, held_ref, swapped_ref, out_ref):
    zones = swapped_ref.shape[0]
    per = out_ref.shape[0] // 2
    _, core, row, _ = place()
    out_ref[...] = steps_ref[...]
    for z in range(zones):
        value = jnp.where(core == 1, held_ref[row * 2 + 2, z], swapped_ref[z])
        for i in range(2):
            out_ref[pl.ds(i * per + z * M + M - 1, 8, stride=zones * M), :] = value[i * 8:(i + 1) * 8]


def states(zones, rows):
    return [pltpu.VMEM((zones + 2, 2 * rows, BLK), BF16)] * 2


HBM = pl.BlockSpec(memory_space=pltpu.HBM)


def call(kernel, name, in_specs, out_shape, scratch, mib, flops, aliases=None):
    return pl.pallas_call(
        kernel,
        in_specs=in_specs,
        out_specs=jax.tree.map(lambda _: VMEM, out_shape),
        out_shape=out_shape,
        scratch_shapes=scratch,
        input_output_aliases=aliases or {},
        compiler_params=pltpu.CompilerParams(vmem_limit_bytes=mib * 2**20),
        cost_estimate=pl.CostEstimate(flops=flops, bytes_accessed=10**6, transcendentals=0),
        name=name,
    )


def body(initial, forcing, fine_blocks, coarse_blocks):
    members, times, cells = forcing.shape
    blocks = cells // BLK
    zones = fine_blocks.shape[0]
    depth = blocks // zones
    rows = members * depth
    count = lax.axis_size("tm")

    force = forcing.reshape(members, times, blocks, BLK).transpose(0, 2, 1, 3).reshape(members * blocks * times, BLK)
    start = initial.reshape(members, blocks, BLK).transpose(1, 0, 2).reshape(blocks * members, BLK)
    fine_blocks = pltpu.with_memory_space_constraint(fine_blocks, pltpu.HBM)
    coarse_blocks = pltpu.with_memory_space_constraint(coarse_blocks, pltpu.HBM)
    weights = jax.ShapeDtypeStruct((zones, 3 * BLK, 2 * BLK), BF16)
    full = jax.ShapeDtypeStruct((zones, rows, BLK), F32)
    held_states = jax.ShapeDtypeStruct((M + 1, zones, rows, BLK), F32)
    held = [pltpu.VMEM(fine_blocks.shape, F32), pltpu.SemaphoreType.DMA((4,))]

    def sent(value, even, odd):
        return lax.ppermute(value, "tm", [(i, (odd if i % 2 else even)(i) % count) for i in range(count)])

    early = [pltpu.VMEM(start.shape, F32), pltpu.VMEM(force.shape, F32), pltpu.SemaphoreType.DMA((2,))]
    late = [pltpu.SemaphoreType.DMA((4,))]
    corner, fine, coarse_blocks = call(
        relax_kernel, "relax", [HBM] * 4, [full, weights, jax.ShapeDtypeStruct(coarse_blocks.shape, F32)],
        states(zones, rows) + held + early + late, 20, 10**9,
    )(pltpu.with_memory_space_constraint(start, pltpu.HBM), pltpu.with_memory_space_constraint(force, pltpu.HBM),
      fine_blocks, coarse_blocks)
    across = {i: i + 1 for i in range(count - 1)}
    across[2], across[count - 1] = 0, 3
    from_chip = lax.ppermute(corner, "tm", list(across.items()))
    from_pair = sent(corner, lambda i: i ^ 1, lambda i: i ^ 1)
    coarse = call(prepare_kernel, "prepare", [VMEM], weights, [], 8, 10**9)(coarse_blocks)
    right = call(
        residual_kernel, "residual", [VMEM] * 6, full,
        states(zones, rows) + [pltpu.VMEM((zones, rows, BLK), F32)], 14, 10**9,
    )(start, from_pair, from_chip, force, fine, coarse)
    def relayed(value, moves):
        target = {i: i ^ 1 for i in range(count)}
        for a, b in moves:
            target.update({2 * a + 1: 2 * b + 1, 2 * b + 1: 2 * b, 2 * b: 2 * a, 2 * a: 2 * a + 1})
        return lax.ppermute(value, "tm", list(target.items()))

    downward = {}
    for i in range(0, count, 4):
        downward.update({i: i ^ 4, i + 1: i + 3, i + 2: i + 1, i + 3: i + 2})
    down = lax.ppermute(right, "tm", list(downward.items()))
    up = relayed(right, [(p + 1, p) for p in range(0, count // 2, 2)])
    near = sent(right, lambda i: i ^ 1, lambda i: i ^ 1)
    far = sent(right, lambda i: i ^ 3, lambda i: i ^ 1)

    def chain(kernel, name, inputs, outputs, held=None):
        return call(
            kernel, name, [VMEM] * (len(inputs) + (held is not None)), [held_states] + [full] * outputs,
            states(zones, rows), 10, 10**9, None if held is None else {len(inputs): 0},
        )(*inputs, *(() if held is None else (held,)))

    def middle(turn, arrivals):
        def kernel(*refs):
            incoming_refs, rest = refs[:arrivals], refs[arrivals:]
            chain_kernel(turn, incoming_refs, *rest[:6], *rest[7:])

        return kernel

    held, following = chain(first_chain_kernel, "chain0", (start, right, from_pair, up, down, coarse), 1)
    incoming = (relayed(following, [(1, 2)]), relayed(following, [(1, 3)]))
    last = count // 4 - 1
    for turn in range(1, last):
        held, following = chain(
            middle(turn, len(incoming)), f"chain{turn}", (*incoming, right, near, far, up, down, coarse), 1, held)
        incoming = (relayed(following, [(2 * turn + y, 2 * turn + 2 + y) for y in range(2)]),)
    held, give = chain(
        functools.partial(enter_kernel, last), "enter", (*incoming, far, down, coarse), 1, held)
    swapped = sent(give, lambda i: i ^ 1, lambda i: i ^ 1)
    held, give = chain(functools.partial(leave_kernel, last), "leave", (right, near, up, coarse), 1, held)
    corners = sent(give, lambda i: i ^ 1, lambda i: i ^ 1)
    forces = jax.ShapeDtypeStruct(force.shape, F32)
    steps = call(final_kernel, "final", [VMEM] * 4, forces, states(zones, rows), 10, 10**9)(held, swapped, force, fine)
    result = call(corners_kernel, "corners", [VMEM] * 3, forces, [], 6, 10**6)(steps, held, corners)
    return result.reshape(members, blocks, times, BLK).transpose(0, 2, 1, 3).reshape(members, times, cells)


def solution(mesh):
    in_specs = (P("grp", None), P("grp", "tm", None), P(), P())
    out_specs = P("grp", "tm", None)
    return jax.shard_map(body, mesh=mesh, in_specs=in_specs, out_specs=out_specs, check_vma=False)
```

```python
import functools

import jax
import jax.numpy as jnp
from jax import lax
from jax.experimental import pallas as pl
from jax.experimental.pallas import tpu as pltpu
from jax.sharding import PartitionSpec as P


M = 4
DELTA = 0.05
BLK = 128
BF16 = jnp.bfloat16
F32 = jnp.float32


def split(value):
    high = value.astype(BF16)
    low = (value - high.astype(F32)).astype(BF16)
    return jnp.concatenate([high, low], axis=0)


def shifted(value, down):
    parts = []
    for part in jnp.split(value, value.shape[0] // 8, axis=0):
        rows = lax.broadcasted_iota(jnp.int32, part.shape, 0)
        moved = pltpu.roll(part, 1 if down else 7, axis=0)
        parts.append(jnp.where(rows == (0 if down else 7), 0.0, moved))
    return jnp.concatenate(parts, axis=0)


def put(state_ref, zone, value):
    zones = state_ref.shape[0] - 2
    state_ref[zone + 1] = split(value)
    if zone == zones - 1:
        state_ref[0] = split(shifted(value, True))
    if zone == 0:
        state_ref[zones + 1] = split(shifted(value, False))


def solve(mixing, step):
    solved = mixing
    for _ in range(2):
        squared = solved * solved
        solved = (mixing + (2.0 * step * solved) * squared) / ((1.0 - step) + (3.0 * step) * squared)
    return solved


def propagate_zone(state_ref, weights_ref, zone, step):
    rows = state_ref.shape[1] // 2
    product = sum(
        jnp.dot(state_ref[zone + k], weights_ref[zone, k * BLK:(k + 1) * BLK], preferred_element_type=F32)
        for k in range(3)
    )
    low, high = product[rows:], product[:rows]
    mixing = high[:, :BLK] + (high[:, BLK:] + (low[:, :BLK] + low[:, BLK:]))
    return solve(mixing, step)


def zone_order(zones, start):
    return [(start + i) % zones for i in range(zones)]


def prepare_zone(block_ref, out_ref, zone):
    for k in range(3):
        turned = block_ref[zone, k].T
        high = turned.astype(BF16)
        out_ref[zone, k * BLK:(k + 1) * BLK, :BLK] = high
        out_ref[zone, k * BLK:(k + 1) * BLK, BLK:] = (turned - high.astype(F32)).astype(BF16)


def fetches(blocks_ref, held_ref, sems):
    count = sems.shape[0]
    size = blocks_ref.shape[0] // count
    spans = [pl.ds(i * size, size) for i in range(count)]
    return [pltpu.make_async_copy(blocks_ref.at[s], held_ref.at[s], sems.at[i]) for i, s in enumerate(spans)]


def prepare_all(copies, held_ref, out_ref):
    size = held_ref.shape[0] // len(copies)
    for i, copy in enumerate(copies):
        copy.wait()
        for z in range(i * size, (i + 1) * size):
            prepare_zone(held_ref, out_ref, z)


def prepare_kernel(blocks_ref, out_ref):
    for z in range(blocks_ref.shape[0]):
        prepare_zone(blocks_ref, out_ref, z)


def place():
    index = lax.axis_index("tm")
    return index, index & 1, (index >> 1) & 1, index >> 2


VMEM = pl.BlockSpec(memory_space=pltpu.VMEM)


def force_rows(force_ref, zone, slot):
    per = force_ref.shape[0] // 2
    zones = per // (M * 8)
    return jnp.concatenate(
        [force_ref[pl.ds(i * per + zone * M + slot, 8, stride=zones * M), :] for i in range(2)], axis=0
    )


def first_rows(initial_ref, zone):
    zones = initial_ref.shape[0] // 16
    return jnp.concatenate([initial_ref[pl.ds(zone * 2 + i, 8, stride=zones * 2), :] for i in range(2)], axis=0)


def relax_kernel(start_ref, given_ref, blocks_ref, next_blocks_ref, out_ref, weights_ref, next_held_ref,
                 state_a, state_b, held_ref, sems, initial_ref, force_ref, early_sems, late_sems):
    zones = weights_ref.shape[0]
    leading = place()[0] == 0
    early = [
        pltpu.make_async_copy(given_ref, force_ref, early_sems.at[0]),
        pltpu.make_async_copy(start_ref, initial_ref, early_sems.at[1]),
    ]
    copies = fetches(blocks_ref, held_ref, sems)
    for copy in early + copies:
        copy.start()
    for copy in early:
        copy.wait()
    for z in range(zones):
        put(state_a, z, force_rows(force_ref, z, 0))
    prepare_all(copies, held_ref, weights_ref)
    late = fetches(next_blocks_ref, next_held_ref, late_sems)
    for copy in late:
        copy.start()

    @pl.when(leading)
    def _():
        for z in range(zones):
            put(state_b, z, first_rows(initial_ref, z))
        for z in range(zones):
            put(state_a, z, propagate_zone(state_b, weights_ref, z, DELTA) + force_rows(force_ref, z, 0))

    source, target = state_a, state_b
    for slot in range(1, M):
        for z in zone_order(zones, slot - 1):
            value = propagate_zone(source, weights_ref, z, DELTA) + force_rows(force_ref, z, slot)
            if slot < M - 1:
                put(target, z, value)
            else:
                out_ref[z] = value
        source, target = target, source
    for copy in late:
        copy.wait()


def residual_kernel(initial_ref, carried_ref, force_ref, fine_ref, coarse_ref, out_ref,
                    state_a, state_b, coarse_part):
    zones = fine_ref.shape[0]
    index = place()[0]
    for z in range(zones):
        put(state_a, z, jnp.where(index == 0, first_rows(initial_ref, z), carried_ref[z]))
    for z in range(zones):
        coarse_part[z] = jnp.where(index < 2, 0.0, propagate_zone(state_a, coarse_ref, z, DELTA * M))
    source, target = state_a, state_b
    for slot in range(M):
        for z in zone_order(zones, slot):
            value = propagate_zone(source, fine_ref, z, DELTA) + force_rows(force_ref, z, slot)
            if slot < M - 1:
                put(target, z, value)
            else:
                out_ref[z] = value - coarse_part[z]
        source, target = target, source


def march(source, target, coarse_ref, held_ref, rights, slot, done=None):
    zones = coarse_ref.shape[0]
    for step, right in enumerate(rights):
        for z in zone_order(zones, step):
            value = propagate_zone(source, coarse_ref, z, DELTA * M) + right(z)
            held_ref[slot + step + 1, z] = value
            if step < len(rights) - 1:
                put(target, z, value)
            elif done is not None:
                done[z] = value
        source, target = target, source


def first_chain_kernel(initial_ref, own_ref, before_ref, coarse_ref, near_ref, first_ref, held_ref, next_ref, state_a, state_b):
    zones = coarse_ref.shape[0]
    _, core, row, plane = place()

    @pl.when((plane == 0) & (core == 1) & (row == 0))
    def _():
        for z in range(zones):
            held_ref[0, z] = first_rows(initial_ref, z)
            held_ref[1, z] = before_ref[z]
            held_ref[2, z] = own_ref[z]

    @pl.when((plane == 0) & (core == 1) & (row == 1))
    def _():
        for z in range(zones):
            held_ref[2, z] = first_ref[z]
            put(state_a, z, first_ref[z])
        march(state_a, state_b, coarse_ref, held_ref, [lambda z: near_ref[z], lambda z: own_ref[z]], 2, next_ref)


def chain_kernel(turn, incoming_refs, own_ref, near_ref, coarse_ref, far_ref, side_ref, held_ref, next_ref,
                 state_a, state_b):
    zones = coarse_ref.shape[0]
    _, core, row, plane = place()
    upper = row == 0
    rights = [
        lambda z: jnp.where(upper, near_ref[z], far_ref[z]),
        lambda z: jnp.where(upper, own_ref[z], side_ref[z]),
        lambda z: jnp.where(upper, far_ref[z], near_ref[z]),
        lambda z: jnp.where(upper, side_ref[z], own_ref[z]),
    ]

    @pl.when((plane == turn) & (core == 1))
    def _():
        for z in range(zones):
            held_ref[0, z] = arrived(incoming_refs, upper, z)
            put(state_a, z, held_ref[0, z])
        march(state_a, state_b, coarse_ref, held_ref, rights, 0, next_ref)


def arrived(incoming_refs, upper, zone):
    if len(incoming_refs) == 1:
        return incoming_refs[0][zone]
    return jnp.where(upper, incoming_refs[0][zone], incoming_refs[1][zone])


def enter_kernel(turn, incoming_ref, far_ref, side_ref, coarse_ref, old_ref, held_ref, give_ref, state_a, state_b):
    del old_ref
    zones = coarse_ref.shape[0]
    _, core, row, plane = place()
    here = (plane == turn) & (core == 1)

    @pl.when(here & (row == 0))
    def _():
        held_ref[0] = incoming_ref[...]

    @pl.when(here & (row == 1))
    def _():
        for z in range(zones):
            put(state_a, z, incoming_ref[z])
        march(state_a, state_b, coarse_ref, held_ref, [lambda z: far_ref[z], lambda z: side_ref[z]], 0)

    give_ref[...] = held_ref[row * 2]


def leave_kernel(turn, own_ref, near_ref, coarse_ref, old_ref, held_ref, give_ref, state_a, state_b):
    zones = coarse_ref.shape[0]
    _, core, row, plane = place()

    @pl.when((plane == turn) & (core == 1))
    def _():
        for z in range(zones):
            put(state_a, z, old_ref[row * 2, z])
        march(state_a, state_b, coarse_ref, held_ref, [lambda z: near_ref[z], lambda z: own_ref[z]], row * 2)

    give_ref[...] = held_ref[row * 2 + 1]


def final_kernel(held_ref, swapped_ref, force_ref, fine_ref, out_ref, state_a, state_b):
    zones = fine_ref.shape[0]
    per = out_ref.shape[0] // 2
    _, core, row, _ = place()
    for z in range(zones):
        put(state_a, z, jnp.where(core == 1, held_ref[row * 2 + 1, z], swapped_ref[z]))
    source, target = state_a, state_b
    for step in range(M - 1):
        for z in zone_order(zones, step):
            value = propagate_zone(source, fine_ref, z, DELTA) + force_rows(force_ref, z, step)
            for i in range(2):
                out_ref[pl.ds(i * per + z * M + step, 8, stride=zones * M), :] = value[i * 8:(i + 1) * 8]
            if step < M - 2:
                put(target, z, value)
        source, target = target, source


def corners_kernel(steps_ref, held_ref, swapped_ref, out_ref):
    zones = swapped_ref.shape[0]
    per = out_ref.shape[0] // 2
    _, core, row, _ = place()
    out_ref[...] = steps_ref[...]
    for z in range(zones):
        value = jnp.where(core == 1, held_ref[row * 2 + 2, z], swapped_ref[z])
        for i in range(2):
            out_ref[pl.ds(i * per + z * M + M - 1, 8, stride=zones * M), :] = value[i * 8:(i + 1) * 8]


def states(zones, rows):
    return [pltpu.VMEM((zones + 2, 2 * rows, BLK), BF16)] * 2


HBM = pl.BlockSpec(memory_space=pltpu.HBM)


def call(kernel, in_specs, out_shape, scratch, mib, flops, aliases=None):
    return pl.pallas_call(
        kernel,
        in_specs=in_specs,
        out_specs=jax.tree.map(lambda _: VMEM, out_shape),
        out_shape=out_shape,
        scratch_shapes=scratch,
        input_output_aliases=aliases or {},
        compiler_params=pltpu.CompilerParams(vmem_limit_bytes=mib * 2**20),
        cost_estimate=pl.CostEstimate(flops=flops, bytes_accessed=10**6, transcendentals=0),
    )


def body(initial, forcing, fine_blocks, coarse_blocks):
    members, times, cells = forcing.shape
    blocks = cells // BLK
    zones = fine_blocks.shape[0]
    depth = blocks // zones
    rows = members * depth
    count = lax.axis_size("tm")

    force = forcing.reshape(members, times, blocks, BLK).transpose(0, 2, 1, 3).reshape(members * blocks * times, BLK)
    start = initial.reshape(members, blocks, BLK).transpose(1, 0, 2).reshape(blocks * members, BLK)
    fine_blocks = pltpu.with_memory_space_constraint(fine_blocks, pltpu.HBM)
    coarse_blocks = pltpu.with_memory_space_constraint(coarse_blocks, pltpu.HBM)
    weights = jax.ShapeDtypeStruct((zones, 3 * BLK, 2 * BLK), BF16)
    full = jax.ShapeDtypeStruct((zones, rows, BLK), F32)
    held_states = jax.ShapeDtypeStruct((M + 1, zones, rows, BLK), F32)
    held = [pltpu.VMEM(fine_blocks.shape, F32), pltpu.SemaphoreType.DMA((4,))]

    def sent(value, even, odd):
        return lax.ppermute(value, "tm", [(i, (odd if i % 2 else even)(i) % count) for i in range(count)])

    early = [pltpu.VMEM(start.shape, F32), pltpu.VMEM(force.shape, F32), pltpu.SemaphoreType.DMA((2,))]
    late = [pltpu.SemaphoreType.DMA((4,))]
    corner, fine, coarse_blocks = call(
        relax_kernel, [HBM] * 4, [full, weights, jax.ShapeDtypeStruct(coarse_blocks.shape, F32)],
        states(zones, rows) + held + early + late, 20, 10**9,
    )(pltpu.with_memory_space_constraint(start, pltpu.HBM), pltpu.with_memory_space_constraint(force, pltpu.HBM),
      fine_blocks, coarse_blocks)
    carried = sent(corner, lambda i: i + 1, lambda i: i + 1)
    coarse = call(prepare_kernel, [VMEM], weights, [], 8, 10**9)(coarse_blocks)
    right = call(
        residual_kernel, [VMEM] * 5, full,
        states(zones, rows) + [pltpu.VMEM((zones, rows, BLK), F32)], 14, 10**9,
    )(start, carried, force, fine, coarse)

    def relayed(value, moves):
        target = {i: i ^ 1 for i in range(count)}
        for a, b in moves:
            target.update({2 * a + 1: 2 * b + 1, 2 * b + 1: 2 * b, 2 * b: 2 * a, 2 * a: 2 * a + 1})
        return lax.ppermute(value, "tm", list(target.items()))

    urgent = {i: i ^ 1 for i in range(count)}
    urgent.update({1: 3, 3: 2, 2: 1, 0: count - 4, count - 4: count - 3, count - 3: 0})
    first = lax.ppermute(right, "tm", list(urgent.items()))
    near = sent(right, lambda i: i ^ 1, lambda i: i ^ 1)
    far = sent(right, lambda i: i ^ 3, lambda i: i ^ 1)

    def chain(kernel, inputs, outputs, held=None):
        return call(
            kernel, [VMEM] * (len(inputs) + (held is not None)), [held_states] + [full] * outputs,
            states(zones, rows), 10, 10**9, None if held is None else {len(inputs): 0},
        )(*inputs, *(() if held is None else (held,)))

    def middle(turn, arrivals):
        def kernel(*refs):
            incoming_refs, rest = refs[5:5 + arrivals], refs[:5] + refs[6 + arrivals:]
            chain_kernel(turn, incoming_refs, *rest)

        return kernel

    held, following = chain(first_chain_kernel, (start, right, carried, coarse, near, first), 1)
    behind, following = lax.optimization_barrier((right, following))
    side = sent(behind, lambda i: i ^ 2, lambda i: i ^ 2)
    across = relayed(following, [(1, 2)])
    along = relayed(following, [(1, 3)])
    incoming = (across, along)
    last = count // 4 - 1
    for turn in range(1, last):
        held, following = chain(
            middle(turn, len(incoming)), (right, near, coarse, far, side, *incoming), 1, held)
        incoming = (relayed(following, [(2 * turn + y, 2 * turn + 2 + y) for y in range(2)]),)
    held, give = chain(
        functools.partial(enter_kernel, last), (*incoming, far, side, coarse), 1, held)
    swapped = sent(give, lambda i: i ^ 1, lambda i: i ^ 1)
    held, give = chain(functools.partial(leave_kernel, last), (right, near, coarse), 1, held)
    corners = sent(give, lambda i: i ^ 1, lambda i: i ^ 1)
    forces = jax.ShapeDtypeStruct(force.shape, F32)
    steps = call(final_kernel, [VMEM] * 4, forces, states(zones, rows), 10, 10**9)(held, swapped, force, fine)
    result = call(corners_kernel, [VMEM] * 3, forces, [], 6, 10**6)(steps, held, corners)
    return result.reshape(members, blocks, times, BLK).transpose(0, 2, 1, 3).reshape(members, times, cells)


def solution(mesh):
    in_specs = (P("grp", None), P("grp", "tm", None), P(), P())
    out_specs = P("grp", "tm", None)
    return jax.shard_map(body, mesh=mesh, in_specs=in_specs, out_specs=out_specs, check_vma=False)
```

```python
import functools

import jax
import jax.numpy as jnp
from jax import lax
from jax.experimental import pallas as pl
from jax.experimental.pallas import tpu as pltpu
from jax.sharding import PartitionSpec as P


M = 4
DELTA = 0.05
BLK = 128
BF16 = jnp.bfloat16
F32 = jnp.float32


def split(value):
    high = value.astype(BF16)
    low = (value - high.astype(F32)).astype(BF16)
    return jnp.concatenate([high, low], axis=0)


def shifted(value, down):
    parts = []
    for part in jnp.split(value, value.shape[0] // 8, axis=0):
        rows = lax.broadcasted_iota(jnp.int32, part.shape, 0)
        moved = pltpu.roll(part, 1 if down else 7, axis=0)
        parts.append(jnp.where(rows == (0 if down else 7), 0.0, moved))
    return jnp.concatenate(parts, axis=0)


def put(state_ref, zone, value):
    zones = state_ref.shape[0] - 2
    state_ref[zone + 1] = split(value)
    if zone == zones - 1:
        state_ref[0] = split(shifted(value, True))
    if zone == 0:
        state_ref[zones + 1] = split(shifted(value, False))


def solve(mixing, step):
    solved = mixing
    for _ in range(2):
        squared = solved * solved
        solved = (mixing + (2.0 * step * solved) * squared) / ((1.0 - step) + (3.0 * step) * squared)
    return solved


def propagate_zone(state_ref, weights_ref, zone, step):
    rows = state_ref.shape[1] // 2
    product = sum(
        jnp.dot(state_ref[zone + k], weights_ref[zone, k * BLK:(k + 1) * BLK], preferred_element_type=F32)
        for k in range(3)
    )
    low, high = product[rows:], product[:rows]
    mixing = high[:, :BLK] + (high[:, BLK:] + (low[:, :BLK] + low[:, BLK:]))
    return solve(mixing, step)


def zone_order(zones, start):
    return [(start + i) % zones for i in range(zones)]


def prepare_zone(block_ref, out_ref, zone):
    for k in range(3):
        turned = block_ref[zone, k].T
        high = turned.astype(BF16)
        out_ref[zone, k * BLK:(k + 1) * BLK, :BLK] = high
        out_ref[zone, k * BLK:(k + 1) * BLK, BLK:] = (turned - high.astype(F32)).astype(BF16)


def fetches(blocks_ref, held_ref, sems):
    count = sems.shape[0]
    size = blocks_ref.shape[0] // count
    spans = [pl.ds(i * size, size) for i in range(count)]
    return [pltpu.make_async_copy(blocks_ref.at[s], held_ref.at[s], sems.at[i]) for i, s in enumerate(spans)]


def prepare_all(copies, held_ref, out_ref):
    size = held_ref.shape[0] // len(copies)
    for i, copy in enumerate(copies):
        copy.wait()
        for z in range(i * size, (i + 1) * size):
            prepare_zone(held_ref, out_ref, z)


def prepare_kernel(blocks_ref, out_ref):
    for z in range(blocks_ref.shape[0]):
        prepare_zone(blocks_ref, out_ref, z)


def place():
    index = lax.axis_index("tm")
    return index, index & 1, (index >> 1) & 1, index >> 2


VMEM = pl.BlockSpec(memory_space=pltpu.VMEM)


def force_rows(force_ref, zone, slot):
    per = force_ref.shape[0] // 2
    zones = per // (M * 8)
    return jnp.concatenate(
        [force_ref[pl.ds(i * per + zone * M + slot, 8, stride=zones * M), :] for i in range(2)], axis=0
    )


def first_rows(initial_ref, zone):
    zones = initial_ref.shape[0] // 16
    return jnp.concatenate([initial_ref[pl.ds(zone * 2 + i, 8, stride=zones * 2), :] for i in range(2)], axis=0)


def relax_kernel(start_ref, given_ref, blocks_ref, next_blocks_ref, out_ref, weights_ref, next_held_ref,
                 state_a, state_b, held_ref, sems, initial_ref, force_ref, early_sems, late_sems):
    zones = weights_ref.shape[0]
    leading = place()[0] == 0
    early = [
        pltpu.make_async_copy(given_ref, force_ref, early_sems.at[0]),
        pltpu.make_async_copy(start_ref, initial_ref, early_sems.at[1]),
    ]
    copies = fetches(blocks_ref, held_ref, sems)
    for copy in early + copies:
        copy.start()
    for copy in early:
        copy.wait()
    for z in range(zones):
        put(state_a, z, force_rows(force_ref, z, 0))
    prepare_all(copies, held_ref, weights_ref)
    late = fetches(next_blocks_ref, next_held_ref, late_sems)
    for copy in late:
        copy.start()

    @pl.when(leading)
    def _():
        for z in range(zones):
            put(state_b, z, first_rows(initial_ref, z))
        for z in range(zones):
            put(state_a, z, propagate_zone(state_b, weights_ref, z, DELTA) + force_rows(force_ref, z, 0))

    source, target = state_a, state_b
    for slot in range(1, M):
        for z in zone_order(zones, slot - 1):
            value = propagate_zone(source, weights_ref, z, DELTA) + force_rows(force_ref, z, slot)
            if slot < M - 1:
                put(target, z, value)
            else:
                out_ref[z] = value
        source, target = target, source
    for copy in late:
        copy.wait()


def residual_kernel(initial_ref, carried_ref, force_ref, fine_ref, coarse_ref, out_ref,
                    state_a, state_b, coarse_part):
    zones = fine_ref.shape[0]
    index = place()[0]
    for z in range(zones):
        put(state_a, z, jnp.where(index == 0, first_rows(initial_ref, z), carried_ref[z]))
    for z in range(zones):
        coarse_part[z] = jnp.where(index < 2, 0.0, propagate_zone(state_a, coarse_ref, z, DELTA * M))
    source, target = state_a, state_b
    for slot in range(M):
        for z in zone_order(zones, slot):
            value = propagate_zone(source, fine_ref, z, DELTA) + force_rows(force_ref, z, slot)
            if slot < M - 1:
                put(target, z, value)
            else:
                out_ref[z] = value - coarse_part[z]
        source, target = target, source


def march(source, target, coarse_ref, held_ref, rights, slot, done=None):
    zones = coarse_ref.shape[0]
    for step, right in enumerate(rights):
        for z in zone_order(zones, step):
            value = propagate_zone(source, coarse_ref, z, DELTA * M) + right(z)
            held_ref[slot + step + 1, z] = value
            if step < len(rights) - 1:
                put(target, z, value)
            elif done is not None:
                done[z] = value
        source, target = target, source


def first_chain_kernel(initial_ref, own_ref, before_ref, coarse_ref, near_ref, first_ref, held_ref, next_ref, state_a, state_b):
    zones = coarse_ref.shape[0]
    _, core, row, plane = place()

    @pl.when((plane == 0) & (core == 1) & (row == 0))
    def _():
        for z in range(zones):
            held_ref[0, z] = first_rows(initial_ref, z)
            held_ref[1, z] = before_ref[z]
            held_ref[2, z] = own_ref[z]

    @pl.when((plane == 0) & (core == 1) & (row == 1))
    def _():
        for z in range(zones):
            held_ref[2, z] = first_ref[z]
            put(state_a, z, first_ref[z])
        march(state_a, state_b, coarse_ref, held_ref, [lambda z: near_ref[z], lambda z: own_ref[z]], 2, next_ref)


def chain_kernel(turn, incoming_refs, own_ref, near_ref, coarse_ref, far_ref, side_ref, held_ref, next_ref,
                 state_a, state_b):
    zones = coarse_ref.shape[0]
    _, core, row, plane = place()
    upper = row == 0
    rights = [
        lambda z: jnp.where(upper, near_ref[z], far_ref[z]),
        lambda z: jnp.where(upper, own_ref[z], side_ref[z]),
        lambda z: jnp.where(upper, far_ref[z], near_ref[z]),
        lambda z: jnp.where(upper, side_ref[z], own_ref[z]),
    ]

    @pl.when((plane == turn) & (core == 1))
    def _():
        for z in range(zones):
            held_ref[0, z] = arrived(incoming_refs, upper, z)
            put(state_a, z, held_ref[0, z])
        march(state_a, state_b, coarse_ref, held_ref, rights, 0, next_ref)


def arrived(incoming_refs, upper, zone):
    if len(incoming_refs) == 1:
        return incoming_refs[0][zone]
    return jnp.where(upper, incoming_refs[0][zone], incoming_refs[1][zone])


def enter_kernel(turn, incoming_ref, far_ref, side_ref, coarse_ref, old_ref, held_ref, give_ref, state_a, state_b):
    del old_ref
    zones = coarse_ref.shape[0]
    _, core, row, plane = place()
    here = (plane == turn) & (core == 1)

    @pl.when(here & (row == 0))
    def _():
        held_ref[0] = incoming_ref[...]

    @pl.when(here & (row == 1))
    def _():
        for z in range(zones):
            put(state_a, z, incoming_ref[z])
        march(state_a, state_b, coarse_ref, held_ref, [lambda z: far_ref[z], lambda z: side_ref[z]], 0)

    give_ref[...] = held_ref[row * 2]


def leave_kernel(turn, own_ref, near_ref, coarse_ref, old_ref, held_ref, give_ref, state_a, state_b):
    zones = coarse_ref.shape[0]
    _, core, row, plane = place()

    @pl.when((plane == turn) & (core == 1))
    def _():
        for z in range(zones):
            put(state_a, z, old_ref[row * 2, z])
        march(state_a, state_b, coarse_ref, held_ref, [lambda z: near_ref[z], lambda z: own_ref[z]], row * 2)

    give_ref[...] = held_ref[row * 2 + 1]


def final_kernel(held_ref, swapped_ref, force_ref, fine_ref, out_ref, state_a, state_b):
    zones = fine_ref.shape[0]
    per = out_ref.shape[0] // 2
    _, core, row, _ = place()
    for z in range(zones):
        put(state_a, z, jnp.where(core == 1, held_ref[row * 2 + 1, z], swapped_ref[z]))
    source, target = state_a, state_b
    for step in range(M - 1):
        for z in zone_order(zones, step):
            value = propagate_zone(source, fine_ref, z, DELTA) + force_rows(force_ref, z, step)
            for i in range(2):
                out_ref[pl.ds(i * per + z * M + step, 8, stride=zones * M), :] = value[i * 8:(i + 1) * 8]
            if step < M - 2:
                put(target, z, value)
        source, target = target, source


def corners_kernel(steps_ref, held_ref, swapped_ref, out_ref):
    zones = swapped_ref.shape[0]
    per = out_ref.shape[0] // 2
    _, core, row, _ = place()
    out_ref[...] = steps_ref[...]
    for z in range(zones):
        value = jnp.where(core == 1, held_ref[row * 2 + 2, z], swapped_ref[z])
        for i in range(2):
            out_ref[pl.ds(i * per + z * M + M - 1, 8, stride=zones * M), :] = value[i * 8:(i + 1) * 8]


def states(zones, rows):
    return [pltpu.VMEM((zones + 2, 2 * rows, BLK), BF16)] * 2


HBM = pl.BlockSpec(memory_space=pltpu.HBM)


def call(kernel, in_specs, out_shape, scratch, mib, flops, aliases=None):
    return pl.pallas_call(
        kernel,
        in_specs=in_specs,
        out_specs=jax.tree.map(lambda _: VMEM, out_shape),
        out_shape=out_shape,
        scratch_shapes=scratch,
        input_output_aliases=aliases or {},
        compiler_params=pltpu.CompilerParams(vmem_limit_bytes=mib * 2**20),
        cost_estimate=pl.CostEstimate(flops=flops, bytes_accessed=10**6, transcendentals=0),
    )


def body(initial, forcing, fine_blocks, coarse_blocks):
    members, times, cells = forcing.shape
    blocks = cells // BLK
    zones = fine_blocks.shape[0]
    depth = blocks // zones
    rows = members * depth
    count = lax.axis_size("tm")

    force = forcing.reshape(members, times, blocks, BLK).transpose(0, 2, 1, 3).reshape(members * blocks * times, BLK)
    start = initial.reshape(members, blocks, BLK).transpose(1, 0, 2).reshape(blocks * members, BLK)
    fine_blocks = pltpu.with_memory_space_constraint(fine_blocks, pltpu.HBM)
    coarse_blocks = pltpu.with_memory_space_constraint(coarse_blocks, pltpu.HBM)
    weights = jax.ShapeDtypeStruct((zones, 3 * BLK, 2 * BLK), BF16)
    full = jax.ShapeDtypeStruct((zones, rows, BLK), F32)
    held_states = jax.ShapeDtypeStruct((M + 1, zones, rows, BLK), F32)
    held = [pltpu.VMEM(fine_blocks.shape, F32), pltpu.SemaphoreType.DMA((4,))]

    def sent(value, even, odd):
        return lax.ppermute(value, "tm", [(i, (odd if i % 2 else even)(i) % count) for i in range(count)])

    early = [pltpu.VMEM(start.shape, F32), pltpu.VMEM(force.shape, F32), pltpu.SemaphoreType.DMA((2,))]
    late = [pltpu.SemaphoreType.DMA((4,))]
    corner, fine, coarse_blocks = call(
        relax_kernel, [HBM] * 4, [full, weights, jax.ShapeDtypeStruct(coarse_blocks.shape, F32)],
        states(zones, rows) + held + early + late, 20, 10**9,
    )(pltpu.with_memory_space_constraint(start, pltpu.HBM), pltpu.with_memory_space_constraint(force, pltpu.HBM),
      fine_blocks, coarse_blocks)
    carried = sent(corner, lambda i: i + 1, lambda i: i + 1)
    coarse = call(prepare_kernel, [VMEM], weights, [], 8, 10**9)(coarse_blocks)
    right = call(
        residual_kernel, [VMEM] * 5, full,
        states(zones, rows) + [pltpu.VMEM((zones, rows, BLK), F32)], 14, 10**9,
    )(start, carried, force, fine, coarse)

    def relayed(value, moves):
        target = {i: i ^ 1 for i in range(count)}
        for a, b in moves:
            target.update({2 * a + 1: 2 * b + 1, 2 * b + 1: 2 * b, 2 * b: 2 * a, 2 * a: 2 * a + 1})
        return lax.ppermute(value, "tm", list(target.items()))

    urgent = {i: i ^ 1 for i in range(count)}
    urgent.update({1: 3, 3: 2, 2: 1, 0: count - 4, count - 4: count - 3, count - 3: 0})
    first = lax.ppermute(right, "tm", list(urgent.items()))
    near = sent(right, lambda i: i ^ 1, lambda i: i ^ 1)
    far = sent(right, lambda i: i ^ 3, lambda i: i ^ 1)

    def chain(kernel, inputs, outputs, held=None):
        return call(
            kernel, [VMEM] * (len(inputs) + (held is not None)), [held_states] + [full] * outputs,
            states(zones, rows), 10, 10**9, None if held is None else {len(inputs): 0},
        )(*inputs, *(() if held is None else (held,)))

    def middle(turn, arrivals):
        def kernel(*refs):
            incoming_refs, rest = refs[5:5 + arrivals], refs[:5] + refs[6 + arrivals:]
            chain_kernel(turn, incoming_refs, *rest)

        return kernel

    held, following = chain(first_chain_kernel, (start, right, carried, coarse, near, first), 1)
    behind, following = lax.optimization_barrier((right, following))
    side = sent(behind, lambda i: i ^ 2, lambda i: i ^ 2)

    def entered(chip):
        target = {i: i ^ 1 for i in range(count)}
        target.update({3: 2 * chip + 1, 2 * chip + 1: 2 * chip, 2 * chip: 3, 2: 0, 0: 1, 1: 2})
        return lax.ppermute(following, "tm", list(target.items()))

    across = entered(2)
    along = entered(3)
    incoming = (across, along)
    last = count // 4 - 1
    for turn in range(1, last):
        held, following = chain(
            middle(turn, len(incoming)), (right, near, coarse, far, side, *incoming), 1, held)
        incoming = (relayed(following, [(2 * turn + y, 2 * turn + 2 + y) for y in range(2)]),)
    held, give = chain(
        functools.partial(enter_kernel, last), (*incoming, far, side, coarse), 1, held)
    swapped = sent(give, lambda i: i ^ 1, lambda i: i ^ 1)
    held, give = chain(functools.partial(leave_kernel, last), (right, near, coarse), 1, held)
    corners = sent(give, lambda i: i ^ 1, lambda i: i ^ 1)
    forces = jax.ShapeDtypeStruct(force.shape, F32)
    steps = call(final_kernel, [VMEM] * 4, forces, states(zones, rows), 10, 10**9)(held, swapped, force, fine)
    result = call(corners_kernel, [VMEM] * 3, forces, [], 6, 10**6)(steps, held, corners)
    return result.reshape(members, blocks, times, BLK).transpose(0, 2, 1, 3).reshape(members, times, cells)


def solution(mesh):
    in_specs = (P("grp", None), P("grp", "tm", None), P(), P())
    out_specs = P("grp", "tm", None)
    return jax.shard_map(body, mesh=mesh, in_specs=in_specs, out_specs=out_specs, check_vma=False)
```

```python
import functools

import jax
import jax.numpy as jnp
from jax import lax
from jax.experimental import pallas as pl
from jax.experimental.pallas import tpu as pltpu
from jax.sharding import PartitionSpec as P


M = 4
DELTA = 0.05
BLK = 128
BF16 = jnp.bfloat16
F32 = jnp.float32


def split(value):
    high = value.astype(BF16)
    low = (value - high.astype(F32)).astype(BF16)
    return jnp.concatenate([high, low], axis=0)


def shifted(value, down):
    parts = []
    for part in jnp.split(value, value.shape[0] // 8, axis=0):
        rows = lax.broadcasted_iota(jnp.int32, part.shape, 0)
        moved = pltpu.roll(part, 1 if down else 7, axis=0)
        parts.append(jnp.where(rows == (0 if down else 7), 0.0, moved))
    return jnp.concatenate(parts, axis=0)


def put(state_ref, zone, value):
    zones = state_ref.shape[0] - 2
    state_ref[zone + 1] = split(value)
    if zone == zones - 1:
        state_ref[0] = split(shifted(value, True))
    if zone == 0:
        state_ref[zones + 1] = split(shifted(value, False))


def solve(mixing, step):
    solved = mixing
    for _ in range(2):
        squared = solved * solved
        solved = (mixing + (2.0 * step * solved) * squared) / ((1.0 - step) + (3.0 * step) * squared)
    return solved


def propagate_zone(state_ref, weights_ref, zone, step):
    rows = state_ref.shape[1] // 2
    product = sum(
        jnp.dot(state_ref[zone + k], weights_ref[zone, k * BLK:(k + 1) * BLK], preferred_element_type=F32)
        for k in range(3)
    )
    low, high = product[rows:], product[:rows]
    mixing = high[:, :BLK] + (high[:, BLK:] + (low[:, :BLK] + low[:, BLK:]))
    return solve(mixing, step)


def zone_order(zones, start):
    return [(start + i) % zones for i in range(zones)]


def prepare_zone(block_ref, out_ref, zone):
    for k in range(3):
        turned = block_ref[zone, k].T
        high = turned.astype(BF16)
        out_ref[zone, k * BLK:(k + 1) * BLK, :BLK] = high
        out_ref[zone, k * BLK:(k + 1) * BLK, BLK:] = (turned - high.astype(F32)).astype(BF16)


def fetches(blocks_ref, held_ref, sems):
    count = sems.shape[0]
    size = blocks_ref.shape[0] // count
    spans = [pl.ds(i * size, size) for i in range(count)]
    return [pltpu.make_async_copy(blocks_ref.at[s], held_ref.at[s], sems.at[i]) for i, s in enumerate(spans)]


def prepare_all(copies, held_ref, out_ref):
    size = held_ref.shape[0] // len(copies)
    for i, copy in enumerate(copies):
        copy.wait()
        for z in range(i * size, (i + 1) * size):
            prepare_zone(held_ref, out_ref, z)


def prepare_kernel(blocks_ref, out_ref):
    for z in range(blocks_ref.shape[0]):
        prepare_zone(blocks_ref, out_ref, z)


def place():
    index = lax.axis_index("tm")
    return index, index & 1, (index >> 1) & 1, index >> 2


VMEM = pl.BlockSpec(memory_space=pltpu.VMEM)


def force_rows(force_ref, zone, slot):
    per = force_ref.shape[0] // 2
    zones = per // (M * 8)
    return jnp.concatenate(
        [force_ref[pl.ds(i * per + zone * M + slot, 8, stride=zones * M), :] for i in range(2)], axis=0
    )


def first_rows(initial_ref, zone):
    zones = initial_ref.shape[0] // 16
    return jnp.concatenate([initial_ref[pl.ds(zone * 2 + i, 8, stride=zones * 2), :] for i in range(2)], axis=0)


def relax_kernel(start_ref, given_ref, blocks_ref, next_blocks_ref, out_ref, weights_ref, next_held_ref,
                 state_a, state_b, held_ref, sems, initial_ref, force_ref, early_sems, late_sems):
    zones = weights_ref.shape[0]
    leading = place()[0] == 0
    early = [
        pltpu.make_async_copy(given_ref, force_ref, early_sems.at[0]),
        pltpu.make_async_copy(start_ref, initial_ref, early_sems.at[1]),
    ]
    copies = fetches(blocks_ref, held_ref, sems)
    for copy in early + copies:
        copy.start()
    for copy in early:
        copy.wait()
    for z in range(zones):
        put(state_a, z, force_rows(force_ref, z, 0))
    prepare_all(copies, held_ref, weights_ref)
    late = fetches(next_blocks_ref, next_held_ref, late_sems)
    for copy in late:
        copy.start()

    @pl.when(leading)
    def _():
        for z in range(zones):
            put(state_b, z, first_rows(initial_ref, z))
        for z in range(zones):
            put(state_a, z, propagate_zone(state_b, weights_ref, z, DELTA) + force_rows(force_ref, z, 0))

    source, target = state_a, state_b
    for slot in range(1, M):
        for z in zone_order(zones, slot - 1):
            value = propagate_zone(source, weights_ref, z, DELTA) + force_rows(force_ref, z, slot)
            if slot < M - 1:
                put(target, z, value)
            else:
                out_ref[z] = value
        source, target = target, source
    for copy in late:
        copy.wait()


def residual_kernel(initial_ref, carried_ref, force_ref, fine_ref, coarse_ref, out_ref,
                    state_a, state_b, coarse_part):
    zones = fine_ref.shape[0]
    index = place()[0]
    for z in range(zones):
        put(state_a, z, jnp.where(index == 0, first_rows(initial_ref, z), carried_ref[z]))
    for z in range(zones):
        coarse_part[z] = jnp.where(index < 2, 0.0, propagate_zone(state_a, coarse_ref, z, DELTA * M))
    source, target = state_a, state_b
    for slot in range(M):
        for z in zone_order(zones, slot):
            value = propagate_zone(source, fine_ref, z, DELTA) + force_rows(force_ref, z, slot)
            if slot < M - 1:
                put(target, z, value)
            else:
                out_ref[z] = value - coarse_part[z]
        source, target = target, source


def march(source, target, coarse_ref, held_ref, rights, slot, done=None):
    zones = coarse_ref.shape[0]
    for step, right in enumerate(rights):
        for z in zone_order(zones, step):
            value = propagate_zone(source, coarse_ref, z, DELTA * M) + right(z)
            held_ref[slot + step + 1, z] = value
            if step < len(rights) - 1:
                put(target, z, value)
            elif done is not None:
                done[z] = value
        source, target = target, source


def first_chain_kernel(initial_ref, own_ref, before_ref, coarse_ref, near_ref, first_ref, held_ref, next_ref, state_a, state_b):
    zones = coarse_ref.shape[0]
    _, core, row, plane = place()

    @pl.when((plane == 0) & (core == 1) & (row == 0))
    def _():
        for z in range(zones):
            held_ref[0, z] = first_rows(initial_ref, z)
            held_ref[1, z] = before_ref[z]
            held_ref[2, z] = own_ref[z]

    @pl.when((plane == 0) & (core == 1) & (row == 1))
    def _():
        for z in range(zones):
            held_ref[2, z] = first_ref[z]
            put(state_a, z, first_ref[z])
        march(state_a, state_b, coarse_ref, held_ref, [lambda z: near_ref[z], lambda z: own_ref[z]], 2, next_ref)


def chain_kernel(turn, incoming_refs, own_ref, near_ref, coarse_ref, far_ref, side_ref, held_ref, next_ref,
                 state_a, state_b):
    zones = coarse_ref.shape[0]
    _, core, row, plane = place()
    upper = row == 0
    rights = [
        lambda z: jnp.where(upper, near_ref[z], far_ref[z]),
        lambda z: jnp.where(upper, own_ref[z], side_ref[z]),
        lambda z: jnp.where(upper, far_ref[z], near_ref[z]),
        lambda z: jnp.where(upper, side_ref[z], own_ref[z]),
    ]

    @pl.when((plane == turn) & (core == 1))
    def _():
        for z in range(zones):
            held_ref[0, z] = arrived(incoming_refs, upper, z)
            put(state_a, z, held_ref[0, z])
        march(state_a, state_b, coarse_ref, held_ref, rights, 0, next_ref)


def arrived(incoming_refs, upper, zone):
    if len(incoming_refs) == 1:
        return incoming_refs[0][zone]
    return jnp.where(upper, incoming_refs[0][zone], incoming_refs[1][zone])


def enter_kernel(turn, incoming_ref, far_ref, side_ref, coarse_ref, old_ref, held_ref, give_ref, state_a, state_b):
    del old_ref
    zones = coarse_ref.shape[0]
    _, core, row, plane = place()
    here = (plane == turn) & (core == 1)

    @pl.when(here & (row == 0))
    def _():
        held_ref[0] = incoming_ref[...]

    @pl.when(here & (row == 1))
    def _():
        for z in range(zones):
            put(state_a, z, incoming_ref[z])
        march(state_a, state_b, coarse_ref, held_ref, [lambda z: far_ref[z], lambda z: side_ref[z]], 0)

    give_ref[...] = held_ref[row * 2]


def leave_kernel(turn, own_ref, near_ref, coarse_ref, old_ref, held_ref, give_ref, state_a, state_b):
    zones = coarse_ref.shape[0]
    _, core, row, plane = place()

    @pl.when((plane == turn) & (core == 1))
    def _():
        for z in range(zones):
            put(state_a, z, old_ref[row * 2, z])
        march(state_a, state_b, coarse_ref, held_ref, [lambda z: near_ref[z], lambda z: own_ref[z]], row * 2)

    give_ref[...] = held_ref[row * 2 + 1]


def final_kernel(held_ref, swapped_ref, force_ref, fine_ref, out_ref, state_a, state_b):
    zones = fine_ref.shape[0]
    per = out_ref.shape[0] // 2
    _, core, row, _ = place()
    for z in range(zones):
        put(state_a, z, jnp.where(core == 1, held_ref[row * 2 + 1, z], swapped_ref[z]))
    source, target = state_a, state_b
    for step in range(M - 1):
        for z in zone_order(zones, step):
            value = propagate_zone(source, fine_ref, z, DELTA) + force_rows(force_ref, z, step)
            for i in range(2):
                out_ref[pl.ds(i * per + z * M + step, 8, stride=zones * M), :] = value[i * 8:(i + 1) * 8]
            if step < M - 2:
                put(target, z, value)
        source, target = target, source


def corners_kernel(steps_ref, held_ref, swapped_ref, out_ref):
    zones = swapped_ref.shape[0]
    per = out_ref.shape[0] // 2
    _, core, row, _ = place()
    out_ref[...] = steps_ref[...]
    for z in range(zones):
        value = jnp.where(core == 1, held_ref[row * 2 + 2, z], swapped_ref[z])
        for i in range(2):
            out_ref[pl.ds(i * per + z * M + M - 1, 8, stride=zones * M), :] = value[i * 8:(i + 1) * 8]


def states(zones, rows):
    return [pltpu.VMEM((zones + 2, 2 * rows, BLK), BF16)] * 2


HBM = pl.BlockSpec(memory_space=pltpu.HBM)


def call(kernel, in_specs, out_shape, scratch, mib, flops, aliases=None):
    return pl.pallas_call(
        kernel,
        in_specs=in_specs,
        out_specs=jax.tree.map(lambda _: VMEM, out_shape),
        out_shape=out_shape,
        scratch_shapes=scratch,
        input_output_aliases=aliases or {},
        compiler_params=pltpu.CompilerParams(vmem_limit_bytes=mib * 2**20),
        cost_estimate=pl.CostEstimate(flops=flops, bytes_accessed=10**6, transcendentals=0),
    )


def body(initial, forcing, fine_blocks, coarse_blocks):
    members, times, cells = forcing.shape
    blocks = cells // BLK
    zones = fine_blocks.shape[0]
    depth = blocks // zones
    rows = members * depth
    count = lax.axis_size("tm")

    force = forcing.reshape(members, times, blocks, BLK).transpose(0, 2, 1, 3).reshape(members * blocks * times, BLK)
    start = initial.reshape(members, blocks, BLK).transpose(1, 0, 2).reshape(blocks * members, BLK)
    fine_blocks = pltpu.with_memory_space_constraint(fine_blocks, pltpu.HBM)
    coarse_blocks = pltpu.with_memory_space_constraint(coarse_blocks, pltpu.HBM)
    weights = jax.ShapeDtypeStruct((zones, 3 * BLK, 2 * BLK), BF16)
    full = jax.ShapeDtypeStruct((zones, rows, BLK), F32)
    held_states = jax.ShapeDtypeStruct((M + 1, zones, rows, BLK), F32)
    held = [pltpu.VMEM(fine_blocks.shape, F32), pltpu.SemaphoreType.DMA((4,))]

    def sent(value, even, odd):
        return lax.ppermute(value, "tm", [(i, (odd if i % 2 else even)(i) % count) for i in range(count)])

    early = [pltpu.VMEM(start.shape, F32), pltpu.VMEM(force.shape, F32), pltpu.SemaphoreType.DMA((2,))]
    late = [pltpu.SemaphoreType.DMA((4,))]
    corner, fine, coarse_blocks = call(
        relax_kernel, [HBM] * 4, [full, weights, jax.ShapeDtypeStruct(coarse_blocks.shape, F32)],
        states(zones, rows) + held + early + late, 20, 10**9,
    )(pltpu.with_memory_space_constraint(start, pltpu.HBM), pltpu.with_memory_space_constraint(force, pltpu.HBM),
      fine_blocks, coarse_blocks)
    carried = sent(corner, lambda i: i + 1, lambda i: i + 1)
    coarse = call(prepare_kernel, [VMEM], weights, [], 8, 10**9)(coarse_blocks)
    right = call(
        residual_kernel, [VMEM] * 5, full,
        states(zones, rows) + [pltpu.VMEM((zones, rows, BLK), F32)], 14, 10**9,
    )(start, carried, force, fine, coarse)

    def relayed(value, moves):
        target = {i: i ^ 1 for i in range(count)}
        for a, b in moves:
            target.update({2 * a + 1: 2 * b + 1, 2 * b + 1: 2 * b, 2 * b: 2 * a, 2 * a: 2 * a + 1})
        return lax.ppermute(value, "tm", list(target.items()))

    urgent = {i: i ^ 1 for i in range(count)}
    urgent.update({1: 3, 3: 2, 2: 1, 0: count - 4, count - 4: count - 3, count - 3: 0})
    first = lax.ppermute(right, "tm", list(urgent.items()))
    near = sent(right, lambda i: i ^ 1, lambda i: i ^ 1)
    far = sent(right, lambda i: i ^ 3, lambda i: i ^ 1)

    def chain(kernel, inputs, outputs, held=None):
        return call(
            kernel, [VMEM] * (len(inputs) + (held is not None)), [held_states] + [full] * outputs,
            states(zones, rows), 10, 10**9, None if held is None else {len(inputs): 0},
        )(*inputs, *(() if held is None else (held,)))

    def middle(turn, arrivals):
        def kernel(*refs):
            incoming_refs, rest = refs[5:5 + arrivals], refs[:5] + refs[6 + arrivals:]
            chain_kernel(turn, incoming_refs, *rest)

        return kernel

    held, following = chain(first_chain_kernel, (start, right, carried, coarse, near, first), 1)
    behind, following = lax.optimization_barrier((right, following))
    side = sent(behind, lambda i: i ^ 2, lambda i: i ^ 2)

    def entered(**moves):
        target = {i: i ^ 1 for i in range(count)}
        target.update({int(i[1:]): to for i, to in moves.items()})
        return lax.ppermute(following, "tm", list(target.items()))

    across = entered(d3=5, d5=4, d4=2, d2=3, d7=11, d11=7, d6=10, d10=6)
    along = entered(d3=7, d7=6, d6=3, d2=0, d0=1, d1=2)
    incoming = (across, along)
    last = count // 4 - 1
    for turn in range(1, last):
        held, following = chain(
            middle(turn, len(incoming)), (right, near, coarse, far, side, *incoming), 1, held)
        incoming = (relayed(following, [(2 * turn + y, 2 * turn + 2 + y) for y in range(2)]),)
    held, give = chain(
        functools.partial(enter_kernel, last), (*incoming, far, side, coarse), 1, held)
    swapped = sent(give, lambda i: i ^ 1, lambda i: i ^ 1)
    held, give = chain(functools.partial(leave_kernel, last), (right, near, coarse), 1, held)
    corners = sent(give, lambda i: i ^ 1, lambda i: i ^ 1)
    forces = jax.ShapeDtypeStruct(force.shape, F32)
    steps = call(final_kernel, [VMEM] * 4, forces, states(zones, rows), 10, 10**9)(held, swapped, force, fine)
    result = call(corners_kernel, [VMEM] * 3, forces, [], 6, 10**6)(steps, held, corners)
    return result.reshape(members, blocks, times, BLK).transpose(0, 2, 1, 3).reshape(members, times, cells)


def solution(mesh):
    in_specs = (P("grp", None), P("grp", "tm", None), P(), P())
    out_specs = P("grp", "tm", None)
    return jax.shard_map(body, mesh=mesh, in_specs=in_specs, out_specs=out_specs, check_vma=False)
```

```python
import functools

import jax
import jax.numpy as jnp
from jax import lax
from jax.experimental import pallas as pl
from jax.experimental.pallas import tpu as pltpu
from jax.sharding import PartitionSpec as P


M = 4
DELTA = 0.05
BLK = 128
BF16 = jnp.bfloat16
F32 = jnp.float32


def split(value):
    high = value.astype(BF16)
    low = (value - high.astype(F32)).astype(BF16)
    return jnp.concatenate([high, low], axis=0)


def shifted(value, down):
    parts = []
    for part in jnp.split(value, value.shape[0] // 8, axis=0):
        rows = lax.broadcasted_iota(jnp.int32, part.shape, 0)
        moved = pltpu.roll(part, 1 if down else 7, axis=0)
        parts.append(jnp.where(rows == (0 if down else 7), 0.0, moved))
    return jnp.concatenate(parts, axis=0)


def put(state_ref, zone, value):
    zones = state_ref.shape[0] - 2
    state_ref[zone + 1] = split(value)
    if zone == zones - 1:
        state_ref[0] = split(shifted(value, True))
    if zone == 0:
        state_ref[zones + 1] = split(shifted(value, False))


def solve(mixing, step):
    solved = mixing
    for _ in range(2):
        squared = solved * solved
        solved = (mixing + (2.0 * step * solved) * squared) / ((1.0 - step) + (3.0 * step) * squared)
    return solved


def propagate_zone(state_ref, weights_ref, zone, step):
    rows = state_ref.shape[1] // 2
    product = sum(
        jnp.dot(state_ref[zone + k], weights_ref[zone, k * BLK:(k + 1) * BLK], preferred_element_type=F32)
        for k in range(3)
    )
    low, high = product[rows:], product[:rows]
    mixing = high[:, :BLK] + (high[:, BLK:] + (low[:, :BLK] + low[:, BLK:]))
    return solve(mixing, step)


def zone_order(zones, start):
    return [(start + i) % zones for i in range(zones)]


def prepare_zone(block_ref, out_ref, zone):
    for k in range(3):
        turned = block_ref[zone, k].T
        high = turned.astype(BF16)
        out_ref[zone, k * BLK:(k + 1) * BLK, :BLK] = high
        out_ref[zone, k * BLK:(k + 1) * BLK, BLK:] = (turned - high.astype(F32)).astype(BF16)


def fetches(blocks_ref, held_ref, sems):
    count = sems.shape[0]
    size = blocks_ref.shape[0] // count
    spans = [pl.ds(i * size, size) for i in range(count)]
    return [pltpu.make_async_copy(blocks_ref.at[s], held_ref.at[s], sems.at[i]) for i, s in enumerate(spans)]


def prepare_all(copies, held_ref, out_ref):
    size = held_ref.shape[0] // len(copies)
    for i, copy in enumerate(copies):
        copy.wait()
        for z in range(i * size, (i + 1) * size):
            prepare_zone(held_ref, out_ref, z)


def prepare_kernel(blocks_ref, out_ref):
    for z in range(blocks_ref.shape[0]):
        prepare_zone(blocks_ref, out_ref, z)


def place():
    index = lax.axis_index("tm")
    return index, index & 1, (index >> 1) & 1, index >> 2


VMEM = pl.BlockSpec(memory_space=pltpu.VMEM)


def force_rows(force_ref, zone, slot):
    per = force_ref.shape[0] // 2
    zones = per // (M * 8)
    return jnp.concatenate(
        [force_ref[pl.ds(i * per + zone * M + slot, 8, stride=zones * M), :] for i in range(2)], axis=0
    )


def first_rows(initial_ref, zone):
    zones = initial_ref.shape[0] // 16
    return jnp.concatenate([initial_ref[pl.ds(zone * 2 + i, 8, stride=zones * 2), :] for i in range(2)], axis=0)


def relax_kernel(start_ref, given_ref, blocks_ref, next_blocks_ref, out_ref, weights_ref, next_held_ref,
                 state_a, state_b, held_ref, sems, initial_ref, force_ref, early_sems, late_sems):
    zones = weights_ref.shape[0]
    leading = place()[0] == 0
    early = [
        pltpu.make_async_copy(given_ref, force_ref, early_sems.at[0]),
        pltpu.make_async_copy(start_ref, initial_ref, early_sems.at[1]),
    ]
    copies = fetches(blocks_ref, held_ref, sems)
    for copy in early + copies:
        copy.start()
    for copy in early:
        copy.wait()
    for z in range(zones):
        put(state_a, z, force_rows(force_ref, z, 0))
    prepare_all(copies, held_ref, weights_ref)
    late = fetches(next_blocks_ref, next_held_ref, late_sems)
    for copy in late:
        copy.start()

    @pl.when(leading)
    def _():
        for z in range(zones):
            put(state_b, z, first_rows(initial_ref, z))
        for z in range(zones):
            put(state_a, z, propagate_zone(state_b, weights_ref, z, DELTA) + force_rows(force_ref, z, 0))

    source, target = state_a, state_b
    for slot in range(1, M):
        for z in zone_order(zones, slot - 1):
            value = propagate_zone(source, weights_ref, z, DELTA) + force_rows(force_ref, z, slot)
            if slot < M - 1:
                put(target, z, value)
            else:
                out_ref[z] = value
        source, target = target, source
    for copy in late:
        copy.wait()


def residual_kernel(initial_ref, carried_ref, force_ref, fine_ref, coarse_ref, out_ref,
                    state_a, state_b, coarse_part):
    zones = fine_ref.shape[0]
    index = place()[0]
    for z in range(zones):
        put(state_a, z, jnp.where(index == 0, first_rows(initial_ref, z), carried_ref[z]))
    for z in range(zones):
        coarse_part[z] = jnp.where(index < 2, 0.0, propagate_zone(state_a, coarse_ref, z, DELTA * M))
    source, target = state_a, state_b
    for slot in range(M):
        for z in zone_order(zones, slot):
            value = propagate_zone(source, fine_ref, z, DELTA) + force_rows(force_ref, z, slot)
            if slot < M - 1:
                put(target, z, value)
            else:
                out_ref[z] = value - coarse_part[z]
        source, target = target, source


def march(source, target, coarse_ref, held_ref, rights, slot, done=None):
    zones = coarse_ref.shape[0]
    for step, right in enumerate(rights):
        for z in zone_order(zones, step):
            value = propagate_zone(source, coarse_ref, z, DELTA * M) + right(z)
            held_ref[slot + step + 1, z] = value
            if step < len(rights) - 1:
                put(target, z, value)
            elif done is not None:
                done[z] = value
        source, target = target, source


def first_chain_kernel(initial_ref, own_ref, before_ref, coarse_ref, near_ref, first_ref, held_ref, next_ref, state_a, state_b):
    zones = coarse_ref.shape[0]
    _, core, row, plane = place()

    @pl.when((plane == 0) & (core == 1) & (row == 0))
    def _():
        for z in range(zones):
            held_ref[0, z] = first_rows(initial_ref, z)
            held_ref[1, z] = before_ref[z]
            held_ref[2, z] = own_ref[z]

    @pl.when((plane == 0) & (core == 1) & (row == 1))
    def _():
        for z in range(zones):
            held_ref[2, z] = first_ref[z]
            put(state_a, z, first_ref[z])
        march(state_a, state_b, coarse_ref, held_ref, [lambda z: near_ref[z], lambda z: own_ref[z]], 2, next_ref)


def chain_kernel(turn, incoming_refs, own_ref, near_ref, coarse_ref, far_ref, side_ref, held_ref, next_ref,
                 state_a, state_b):
    zones = coarse_ref.shape[0]
    _, core, row, plane = place()
    upper = row == 0
    rights = [
        lambda z: jnp.where(upper, near_ref[z], far_ref[z]),
        lambda z: jnp.where(upper, own_ref[z], side_ref[z]),
        lambda z: jnp.where(upper, far_ref[z], near_ref[z]),
        lambda z: jnp.where(upper, side_ref[z], own_ref[z]),
    ]

    @pl.when((plane == turn) & (core == 1))
    def _():
        for z in range(zones):
            held_ref[0, z] = arrived(incoming_refs, upper, z)
            put(state_a, z, held_ref[0, z])
        march(state_a, state_b, coarse_ref, held_ref, rights, 0, next_ref)


def arrived(incoming_refs, upper, zone):
    if len(incoming_refs) == 1:
        return incoming_refs[0][zone]
    return jnp.where(upper, incoming_refs[0][zone], incoming_refs[1][zone])


def enter_kernel(turn, incoming_ref, far_ref, side_ref, coarse_ref, old_ref, held_ref, give_ref, state_a, state_b):
    del old_ref
    zones = coarse_ref.shape[0]
    _, core, row, plane = place()
    here = (plane == turn) & (core == 1)

    @pl.when(here & (row == 0))
    def _():
        held_ref[0] = incoming_ref[...]

    @pl.when(here & (row == 1))
    def _():
        for z in range(zones):
            put(state_a, z, incoming_ref[z])
        march(state_a, state_b, coarse_ref, held_ref, [lambda z: far_ref[z], lambda z: side_ref[z]], 0)

    give_ref[...] = held_ref[row * 2]


def leave_kernel(turn, own_ref, near_ref, coarse_ref, old_ref, held_ref, give_ref, state_a, state_b):
    zones = coarse_ref.shape[0]
    _, core, row, plane = place()

    @pl.when((plane == turn) & (core == 1))
    def _():
        for z in range(zones):
            put(state_a, z, old_ref[row * 2, z])
        march(state_a, state_b, coarse_ref, held_ref, [lambda z: near_ref[z], lambda z: own_ref[z]], row * 2)

    give_ref[...] = held_ref[row * 2 + 1]


def final_kernel(held_ref, swapped_ref, force_ref, fine_ref, out_ref, state_a, state_b):
    zones = fine_ref.shape[0]
    per = out_ref.shape[0] // 2
    _, core, row, _ = place()
    for z in range(zones):
        put(state_a, z, jnp.where(core == 1, held_ref[row * 2 + 1, z], swapped_ref[z]))
    source, target = state_a, state_b
    for step in range(M - 1):
        for z in zone_order(zones, step):
            value = propagate_zone(source, fine_ref, z, DELTA) + force_rows(force_ref, z, step)
            for i in range(2):
                out_ref[pl.ds(i * per + z * M + step, 8, stride=zones * M), :] = value[i * 8:(i + 1) * 8]
            if step < M - 2:
                put(target, z, value)
        source, target = target, source


def corners_kernel(steps_ref, held_ref, swapped_ref, out_ref):
    zones = swapped_ref.shape[0]
    per = out_ref.shape[0] // 2
    _, core, row, _ = place()
    out_ref[...] = steps_ref[...]
    for z in range(zones):
        value = jnp.where(core == 1, held_ref[row * 2 + 2, z], swapped_ref[z])
        for i in range(2):
            out_ref[pl.ds(i * per + z * M + M - 1, 8, stride=zones * M), :] = value[i * 8:(i + 1) * 8]


def states(zones, rows):
    return [pltpu.VMEM((zones + 2, 2 * rows, BLK), BF16)] * 2


HBM = pl.BlockSpec(memory_space=pltpu.HBM)


def call(kernel, in_specs, out_shape, scratch, mib, flops, aliases=None):
    return pl.pallas_call(
        kernel,
        in_specs=in_specs,
        out_specs=jax.tree.map(lambda _: VMEM, out_shape),
        out_shape=out_shape,
        scratch_shapes=scratch,
        input_output_aliases=aliases or {},
        compiler_params=pltpu.CompilerParams(vmem_limit_bytes=mib * 2**20),
        cost_estimate=pl.CostEstimate(flops=flops, bytes_accessed=10**6, transcendentals=0),
    )


def body(initial, forcing, fine_blocks, coarse_blocks):
    members, times, cells = forcing.shape
    blocks = cells // BLK
    zones = fine_blocks.shape[0]
    depth = blocks // zones
    rows = members * depth
    count = lax.axis_size("tm")

    force = forcing.reshape(members, times, blocks, BLK).transpose(0, 2, 1, 3).reshape(members * blocks * times, BLK)
    start = initial.reshape(members, blocks, BLK).transpose(1, 0, 2).reshape(blocks * members, BLK)
    fine_blocks = pltpu.with_memory_space_constraint(fine_blocks, pltpu.HBM)
    coarse_blocks = pltpu.with_memory_space_constraint(coarse_blocks, pltpu.HBM)
    weights = jax.ShapeDtypeStruct((zones, 3 * BLK, 2 * BLK), BF16)
    full = jax.ShapeDtypeStruct((zones, rows, BLK), F32)
    held_states = jax.ShapeDtypeStruct((M + 1, zones, rows, BLK), F32)
    held = [pltpu.VMEM(fine_blocks.shape, F32), pltpu.SemaphoreType.DMA((4,))]

    def sent(value, even, odd):
        return lax.ppermute(value, "tm", [(i, (odd if i % 2 else even)(i) % count) for i in range(count)])

    early = [pltpu.VMEM(start.shape, F32), pltpu.VMEM(force.shape, F32), pltpu.SemaphoreType.DMA((2,))]
    late = [pltpu.SemaphoreType.DMA((4,))]
    corner, fine, coarse_blocks = call(
        relax_kernel, [HBM] * 4, [full, weights, jax.ShapeDtypeStruct(coarse_blocks.shape, F32)],
        states(zones, rows) + held + early + late, 20, 10**9,
    )(pltpu.with_memory_space_constraint(start, pltpu.HBM), pltpu.with_memory_space_constraint(force, pltpu.HBM),
      fine_blocks, coarse_blocks)
    carried = sent(corner, lambda i: i + 1, lambda i: i + 1)
    coarse = call(prepare_kernel, [VMEM], weights, [], 8, 10**9)(coarse_blocks)
    right = call(
        residual_kernel, [VMEM] * 5, full,
        states(zones, rows) + [pltpu.VMEM((zones, rows, BLK), F32)], 14, 10**9,
    )(start, carried, force, fine, coarse)

    def relayed(value, turn):
        target = {i: i ^ 1 for i in range(count)}
        for i in (4 * turn, 4 * turn + 2):
            target.update({i + 1: i + 5, i + 5: i + 4, i + 4: i + 1, i: i ^ 2})
        return lax.ppermute(value, "tm", list(target.items()))

    urgent = {i: i ^ 1 for i in range(count)}
    urgent.update({1: 3, 3: 2, 2: 1, 0: count - 4, count - 4: count - 3, count - 3: 0})
    first = lax.ppermute(right, "tm", list(urgent.items()))
    near = sent(right, lambda i: i ^ 1, lambda i: i ^ 1)
    far = sent(right, lambda i: i ^ 3, lambda i: i ^ 1)

    def chain(kernel, inputs, outputs, held=None):
        return call(
            kernel, [VMEM] * (len(inputs) + (held is not None)), [held_states] + [full] * outputs,
            states(zones, rows), 10, 10**9, None if held is None else {len(inputs): 0},
        )(*inputs, *(() if held is None else (held,)))

    def middle(turn, arrivals):
        def kernel(*refs):
            incoming_refs, rest = refs[5:5 + arrivals], refs[:5] + refs[6 + arrivals:]
            chain_kernel(turn, incoming_refs, *rest)

        return kernel

    held, following = chain(first_chain_kernel, (start, right, carried, coarse, near, first), 1)
    behind, following = lax.optimization_barrier((right, following))
    side = sent(behind, lambda i: i ^ 2, lambda i: i ^ 2)

    def entered(**moves):
        target = {i: i ^ 1 for i in range(count)}
        target.update({int(i[1:]): to for i, to in moves.items()})
        return lax.ppermute(following, "tm", list(target.items()))

    across = entered(d3=5, d5=4, d4=2, d2=3, d7=11, d11=7, d6=10, d10=6)
    along = entered(d3=7, d7=6, d6=3, d2=0, d0=1, d1=2)
    incoming = (across, along)
    last = count // 4 - 1
    for turn in range(1, last):
        held, following = chain(
            middle(turn, len(incoming)), (right, near, coarse, far, side, *incoming), 1, held)
        incoming = (relayed(following, turn),)
    held, give = chain(
        functools.partial(enter_kernel, last), (*incoming, far, side, coarse), 1, held)
    swapped = sent(give, lambda i: i ^ 1, lambda i: i ^ 1)
    held, give = chain(functools.partial(leave_kernel, last), (right, near, coarse), 1, held)
    corners = sent(give, lambda i: i ^ 1, lambda i: i ^ 1)
    forces = jax.ShapeDtypeStruct(force.shape, F32)
    steps = call(final_kernel, [VMEM] * 4, forces, states(zones, rows), 10, 10**9)(held, swapped, force, fine)
    result = call(corners_kernel, [VMEM] * 3, forces, [], 6, 10**6)(steps, held, corners)
    return result.reshape(members, blocks, times, BLK).transpose(0, 2, 1, 3).reshape(members, times, cells)


def solution(mesh):
    in_specs = (P("grp", None), P("grp", "tm", None), P(), P())
    out_specs = P("grp", "tm", None)
    return jax.shard_map(body, mesh=mesh, in_specs=in_specs, out_specs=out_specs, check_vma=False)
```
